32 devices in a mesh: seq: 8 (over y, x, core), head: 4 (over z).
Axes of the slice: x: 2, y: 2, z: 4, core: 2. Of those that a mesh axis runs over, the one named last changes fastest.
Arguments:
- queries: bfloat16 [1024, 1024], P('seq', 'head'), may hold values from -24 to 24
- keys_values: bfloat16 [2, 1024, 128], P(None, 'seq'), may hold values from -6 to 6
- out_weight: bfloat16 [2560, 8, 128], P('head'), may hold values from -0.125 to 0.125
- out_grad: bfloat16 [1024, 2560], P('seq'), may hold values from -6 to 6
- positions: int32 [1024], replicated, may hold values from 0 to 1023, as said below
Outputs:
- d_query: bfloat16 [1024, 1024], P('seq', 'head')
- d_out_weight: float32 [2560, 8, 128], P('seq', 'head')
The draws below stay inside these ranges and needn't reach their ends.
Inputs may be any that keep to these rules, and one draw needn't show every extreme that they name: positions holds each of 0 to 1023 once, in runs of 64 consecutive rows with consecutive positions, each run starting at a row and a position that are multiples of 64.
All inputs are finite; a program needn't handle non-finite values.
Results may differ from the reference program's by a relative error of at most 0.007.
Values may be sent and summed in bfloat16 or wider, within the bound.
No kernel may reach another device: no remote copies, remote signals or barrier semaphores. Data moves between devices by JAX's collectives and lax.ppermute only.
A program may use at most 64 MiB of HBM per device.

```python
import jax
import jax.numpy as jnp
from jax import lax

HD = 128
GROUP = 8
DW = 2560
TOK_DEV = 128
HQ = 8
KVH = 1
SEQ = 1024


def raw_pairs(key):
    base = jax.random.fold_in(key, 11)
    raw = jnp.clip(jax.random.normal(base, (2, SEQ, KVH * HD), jnp.float32), -6.0, 6.0)
    return raw


def draw_keys_values(key, part):
    raw = raw_pairs(key)
    return raw.astype(jnp.bfloat16)


def draw_queries(key, part):
    qkey = jax.random.fold_in(key, 23)
    base = jnp.clip(jax.random.normal(qkey, (SEQ, HQ, HD), jnp.float32), -6.0, 6.0)
    return base.reshape(SEQ, HQ * HD).astype(jnp.bfloat16)


def draw_positions(key, part):
    runs = 2 * SEQ // TOK_DEV
    half_run = TOK_DEV // 2
    order = jax.random.permutation(jax.random.fold_in(key, 41), runs).astype(jnp.int32)
    within = jnp.arange(half_run, dtype=jnp.int32)
    return (order[:, None] * half_run + within[None, :]).reshape(SEQ).astype(jnp.int32)


def with_spikes(array, key, source, target, shards_of, factor):
    owner, partner = [(jnp.arange(array.shape[position]) // (array.shape[position] // shards_of)).reshape([-1 if axis == position else 1 for axis in range(array.ndim)]) for position in (source, target)]
    chosen = jax.random.permutation(key, shards_of)[partner]
    strong = (owner == chosen) | (owner == (partner + shards_of // 2) % shards_of)
    return jnp.where(strong, factor * array, array)


def shard_levels(own_key, shape, cuts, least, top_value):
    loudness, own = 1.0, jax.random.fold_in(own_key, 6)
    for dim, blocks in cuts:
        heights = jnp.exp(jax.random.uniform(jax.random.fold_in(own, dim), (blocks,), jnp.float32, least / len(cuts), top_value / len(cuts)))
        loudness = loudness * jnp.repeat(heights, shape[dim] // blocks).reshape([-1 if axis == dim else 1 for axis in range(len(shape))])
    return loudness


def noise(key, dims, deviation, bound, pieces=(), kind=jnp.bfloat16):
    values = deviation * jax.random.normal(key, dims, jnp.float32)
    if pieces:
        values = values * shard_levels(key, dims, pieces, -0.22, 0.18)
    return jnp.clip(values, -bound, bound).astype(kind)


def bell_draw_with(key, dims, spread, most, cuts, heavy, kind=jnp.bfloat16):
    array = spread * jax.random.normal(key, dims, jnp.float32)
    if cuts:
        array = array * shard_levels(key, dims, cuts, -0.22, 0.18)
    return jnp.clip(with_spikes(array, jax.random.fold_in(key, 3), *heavy), -most, most).astype(kind)


def setup_inputs(seed: int = 0) -> dict:
    splits = jax.random.split(jax.random.key(seed), 6)
    return {
        "queries": draw_queries(jax.random.fold_in(splits[5], 71), 0),
        "keys_values": draw_keys_values(jax.random.fold_in(splits[5], 71), 0),
        "out_weight": noise(splits[2], (DW, HQ, HD), DW ** -0.5, 0.125, ((0, 4),)),
        "out_grad": bell_draw_with(splits[3], (SEQ, DW), 1.0, 6.0, ((0, 8),), (0, 1, 8, 2.0)),
        "positions": draw_positions(jax.random.fold_in(splits[5], 71), 0),
    }


big_negative = -1.0e30


def reference(queries, keys_values, out_weight, out_grad, positions):
    scale = HD ** -0.5
    d_attn = jnp.dot(out_grad, out_weight.reshape(DW, HQ * HD), preferred_element_type=jnp.float32).astype(jnp.bfloat16)
    query_heads = queries.reshape(SEQ, HQ, HD).transpose(1, 0, 2)
    grad_heads = d_attn.reshape(SEQ, HQ, HD).transpose(1, 0, 2)
    key_heads = jnp.repeat(keys_values[0].reshape(SEQ, KVH, HD).transpose(1, 0, 2), GROUP, axis=0)
    value_heads = jnp.repeat(keys_values[1].reshape(SEQ, KVH, HD).transpose(1, 0, 2), GROUP, axis=0)
    visible = positions[None, :] <= positions[:, None]

    def one_head(operands):
        query, key, value, grad = operands
        scores = jnp.dot(query, key.T, preferred_element_type=jnp.float32) * scale
        scores = jnp.where(visible, scores, big_negative)
        top = jnp.max(scores, axis=1, keepdims=True)
        weights = jnp.where(visible, jnp.exp(scores - top), 0.0)
        probs = weights / jnp.sum(weights, axis=1, keepdims=True)
        attn_full = jnp.dot(probs.astype(jnp.bfloat16), value, preferred_element_type=jnp.float32)
        delta = jnp.sum(grad.astype(jnp.float32) * attn_full, axis=1, keepdims=True)
        dprob = jnp.dot(grad, value.T, preferred_element_type=jnp.float32)
        dscore = (probs * (dprob - delta)).astype(jnp.bfloat16)
        dquery = jnp.dot(dscore, key, preferred_element_type=jnp.float32) * scale
        return attn_full.astype(jnp.bfloat16), dquery.astype(jnp.bfloat16)

    attn, d_query = lax.map(one_head, (query_heads, key_heads, value_heads, grad_heads))
    attn = attn.transpose(1, 0, 2).reshape(SEQ, HQ * HD)
    d_query = d_query.transpose(1, 0, 2).reshape(SEQ, HQ * HD)
    d_out_weight = lax.dot_general(out_grad, attn, (((0,), (0,)), ((), ())), preferred_element_type=jnp.float32)
    return d_query, d_out_weight.reshape(DW, HQ, HD)
```

```python
import math

import jax
import jax.numpy as jnp
from jax import lax
from jax.sharding import PartitionSpec as P

HD = 128
GROUP = 8


big_negative = -1e30


def attend_block(query_rows, query_pos, block_kv, key_pos, scale):
    scores = (
        lax.dot_general(
            query_rows, block_kv[0], (((1,), (1,)), ((), ())), preferred_element_type=jnp.float32
        )
        * scale
    )
    visible = key_pos[None, :] <= query_pos[:, None]
    return (jnp.where(visible, scores, big_negative), visible)


def sweep(step_fn, states, key_piece, offset, positions):
    span_size = key_piece.shape[1]
    block_size = math.gcd(span_size, 1024)

    def step(step_index, inner):
        block_kv = lax.dynamic_slice_in_dim(key_piece, step_index * block_size, block_size, 1)
        key_pos = lax.dynamic_slice_in_dim(
            positions, offset + step_index * block_size, block_size, 0
        )
        return step_fn(inner, block_kv, key_pos)

    return lax.fori_loop(0, span_size // block_size, step, states)


def wide_body(queries, keys_values, out_weight, out_grad, positions):
    token_count = queries.shape[0]
    head_count = queries.shape[1] // HD
    scale = HD ** (-0.5)
    seq_index = lax.axis_index("seq")
    head_index = lax.axis_index("head")
    kv_group = head_index * head_count // GROUP
    own_kv = lax.dynamic_slice_in_dim(keys_values, kv_group * HD, HD, 2)
    own_pos = lax.dynamic_slice_in_dim(positions, seq_index * token_count, token_count, 0)
    query_pos = jnp.repeat(own_pos, head_count)
    query_rows = queries.reshape(token_count * head_count, HD)
    d_attn = jnp.einsum(
        "td,dhc->thc",
        out_grad,
        lax.all_to_all(out_weight, "head", split_axis=1, concat_axis=0, tiled=True),
        preferred_element_type=jnp.float32,
    )
    d_attn = d_attn.astype(jnp.bfloat16).reshape(token_count * head_count, HD)
    row_total = token_count * head_count
    zeros_col = jnp.zeros((row_total, 1), jnp.float32)
    zeros_rows = jnp.zeros((row_total, HD), jnp.float32)
    lowest_col = jnp.full((row_total, 1), big_negative, jnp.float32)
    all_kv = lax.all_gather(own_kv, "seq", axis=1, tiled=True)

    def run_sweep(step_fn, init):
        return sweep(step_fn, init, all_kv, 0, positions)

    def stats_step(states, block_kv, key_pos):
        top, norm = states
        scores, visible = attend_block(query_rows, query_pos, block_kv, key_pos, scale)
        new_top = jnp.maximum(top, jnp.max(scores, axis=1, keepdims=True))
        weights = jnp.where(visible, jnp.exp(scores - new_top), 0.0)
        norm = jnp.exp(top - new_top) * norm + jnp.sum(weights, axis=1, keepdims=True)
        return (new_top, norm)

    top, norm = run_sweep(stats_step, (lowest_col, zeros_col))

    def block_probs(block_kv, key_pos):
        scores, visible = attend_block(query_rows, query_pos, block_kv, key_pos, scale)
        return jnp.where(visible, jnp.exp(scores - top), 0.0) / norm

    def out_step(acc_out, block_kv, key_pos):
        probs = block_probs(block_kv, key_pos)
        return acc_out + jnp.dot(
            probs.astype(jnp.bfloat16), block_kv[1], preferred_element_type=jnp.float32
        )

    attn_full = run_sweep(out_step, zeros_rows)
    delta = jnp.sum(d_attn.astype(jnp.float32) * attn_full, axis=1, keepdims=True)

    def grad_step(acc_grad, block_kv, key_pos):
        probs = block_probs(block_kv, key_pos)
        dprob = lax.dot_general(
            d_attn, block_kv[1], (((1,), (1,)), ((), ())), preferred_element_type=jnp.float32
        )
        dscore = (probs * (dprob - delta)).astype(jnp.bfloat16)
        return acc_grad + jnp.dot(dscore, block_kv[0], preferred_element_type=jnp.float32)

    d_rows = run_sweep(grad_step, zeros_rows) * scale
    attn = attn_full.astype(jnp.bfloat16).reshape(token_count, head_count, HD)
    d_query = d_rows.astype(jnp.bfloat16).reshape(token_count, head_count * HD)
    d_out_weight = lax.psum_scatter(
        jnp.einsum("td,thc->dhc", out_grad, attn, preferred_element_type=jnp.float32),
        "seq",
        scatter_dimension=0,
        tiled=True,
    )
    return (d_query, d_out_weight)


def xor_pairs(size, mask):
    return [(index, index ^ mask) for index in range(size)]


def narrow_body(queries, keys_values, out_weight, out_grad, positions, seq_size, head_size):
    token_count = queries.shape[0]
    head_count = queries.shape[1] // HD
    width = head_count * HD
    scale = HD ** (-0.5)
    seq_index = lax.axis_index("seq")
    head_index = lax.axis_index("head")
    pair_index = seq_index // 2
    pair_count = seq_size // 2
    kv_group = head_index * head_count // GROUP
    own_kv = lax.dynamic_slice_in_dim(keys_values, kv_group * HD, HD, 2)
    span = out_grad.shape[1] // pair_count
    rows_in = out_weight.shape[0]

    own_tokens = jnp.concatenate([own_kv[0], own_kv[1], queries], axis=1)
    tokens = [own_tokens] + [
        lax.ppermute(own_tokens, "seq", xor_pairs(seq_size, 2 * mask))
        for mask in range(1, pair_count)
    ]
    grads = []
    for mask in range(pair_count):
        piece = lax.dynamic_slice_in_dim(out_grad, (pair_index ^ mask) * span, span, 1)
        if mask:
            piece = lax.ppermute(piece, "seq", xor_pairs(seq_size, 2 * mask))
        grads.append(piece)

    own_cols = lax.dynamic_slice_in_dim(out_grad, head_index * rows_in, rows_in, 1)
    parts = jnp.einsum("td,dhc->thc", own_cols, out_weight, preferred_element_type=jnp.float32)
    parts = parts.astype(jnp.bfloat16).reshape(token_count, head_size * width)
    d_attn = 0.0
    for mask in range(head_size):
        part = lax.dynamic_slice_in_dim(parts, (head_index ^ mask) * width, width, 1)
        if mask:
            part = lax.ppermute(part, "head", xor_pairs(head_size, mask))
        d_attn = d_attn + part.astype(jnp.float32)
    d_attn = d_attn.astype(jnp.bfloat16)

    tokens = jnp.concatenate(tokens, axis=0)
    near_kv = tokens[:, : 2 * HD]
    far_kv = lax.ppermute(near_kv, "seq", xor_pairs(seq_size, 1))
    kv = jnp.concatenate([near_kv, far_kv], axis=0)
    keys, values = kv[:, :HD], kv[:, HD:]

    def places(low):
        return jnp.concatenate(
            [
                lax.dynamic_slice_in_dim(
                    positions, (2 * (pair_index ^ mask) + low) * token_count, token_count, 0
                )
                for mask in range(pair_count)
            ]
        )

    low = seq_index % 2
    query_pos = places(low)
    key_pos = jnp.concatenate([query_pos, places(1 - low)])
    visible = key_pos[None, :] <= query_pos[:, None]
    attn, d_query = [], []
    for head in range(head_count):
        query = tokens[:, 2 * HD + head * HD : 2 * HD + (head + 1) * HD]
        scores = (
            lax.dot_general(query, keys, (((1,), (1,)), ((), ())), preferred_element_type=jnp.float32)
            * scale
        )
        scores = jnp.where(visible, scores, big_negative)
        top = jnp.max(scores, axis=1, keepdims=True)
        weights = jnp.where(visible, jnp.exp(scores - top), 0.0)
        probs = weights / jnp.sum(weights, axis=1, keepdims=True)
        full = jnp.dot(probs.astype(jnp.bfloat16), values, preferred_element_type=jnp.float32)
        attn.append(full.astype(jnp.bfloat16))
        grad = d_attn[:, head * HD : (head + 1) * HD]
        delta = jnp.sum(grad.astype(jnp.float32) * full[:token_count], axis=1, keepdims=True)
        dprob = lax.dot_general(
            grad, values, (((1,), (1,)), ((), ())), preferred_element_type=jnp.float32
        )
        dscore = (probs[:token_count] * (dprob - delta)).astype(jnp.bfloat16)
        d_query.append(
            (jnp.dot(dscore, keys, preferred_element_type=jnp.float32) * scale).astype(jnp.bfloat16)
        )
    d_query = jnp.concatenate(d_query, axis=1)
    attn = jnp.concatenate(attn, axis=1)
    grads = jnp.concatenate(grads, axis=0)
    sums = lax.dot_general(
        grads, attn, (((0,), (0,)), ((), ())), preferred_element_type=jnp.float32
    )
    half = span // 2
    mine = lax.dynamic_slice_in_dim(sums, low * half, half, 0)
    theirs = lax.dynamic_slice_in_dim(sums, (1 - low) * half, half, 0)
    mine = mine + lax.ppermute(theirs, "seq", xor_pairs(seq_size, 1))
    return (d_query, mine.reshape(half, head_count, HD))


def solution(mesh):
    seq_size, head_size = mesh.shape["seq"], mesh.shape["head"]
    if seq_size in (2, 4, 8) and head_size & (head_size - 1) == 0:

        def body(*arrays):
            return narrow_body(*arrays, seq_size, head_size)

    else:
        body = wide_body
    return jax.shard_map(
        body,
        mesh=mesh,
        in_specs=(
            P("seq", "head"),
            P(None, "seq", None),
            P("head", None, None),
            P("seq", None),
            P(),
        ),
        out_specs=(P("seq", "head"), P("seq", "head", None)),
        check_vma=False,
    )
```

```python
import math

import jax
import jax.numpy as jnp
from jax import lax
from jax.experimental import pallas as pl
from jax.experimental.pallas import tpu as pltpu
from jax.sharding import PartitionSpec as P


HD = 128
GROUP = 8


big_negative = -1e30


def attend_block(query_rows, query_pos, block_kv, key_pos, scale):
    scores = (
        lax.dot_general(
            query_rows, block_kv[0], (((1,), (1,)), ((), ())), preferred_element_type=jnp.float32
        )
        * scale
    )
    visible = key_pos[None, :] <= query_pos[:, None]
    return (jnp.where(visible, scores, big_negative), visible)


def sweep(step_fn, states, key_piece, offset, positions):
    span_size = key_piece.shape[1]
    block_size = math.gcd(span_size, 1024)

    def step(step_index, inner):
        block_kv = lax.dynamic_slice_in_dim(key_piece, step_index * block_size, block_size, 1)
        key_pos = lax.dynamic_slice_in_dim(
            positions, offset + step_index * block_size, block_size, 0
        )
        return step_fn(inner, block_kv, key_pos)

    return lax.fori_loop(0, span_size // block_size, step, states)


def wide_body(queries, keys_values, out_weight, out_grad, positions):
    token_count = queries.shape[0]
    head_count = queries.shape[1] // HD
    scale = HD ** (-0.5)
    seq_index = lax.axis_index("seq")
    head_index = lax.axis_index("head")
    kv_group = head_index * head_count // GROUP
    own_kv = lax.dynamic_slice_in_dim(keys_values, kv_group * HD, HD, 2)
    own_pos = lax.dynamic_slice_in_dim(positions, seq_index * token_count, token_count, 0)
    query_pos = jnp.repeat(own_pos, head_count)
    query_rows = queries.reshape(token_count * head_count, HD)
    d_attn = jnp.einsum(
        "td,dhc->thc",
        out_grad,
        lax.all_to_all(out_weight, "head", split_axis=1, concat_axis=0, tiled=True),
        preferred_element_type=jnp.float32,
    )
    d_attn = d_attn.astype(jnp.bfloat16).reshape(token_count * head_count, HD)
    row_total = token_count * head_count
    zeros_col = jnp.zeros((row_total, 1), jnp.float32)
    zeros_rows = jnp.zeros((row_total, HD), jnp.float32)
    lowest_col = jnp.full((row_total, 1), big_negative, jnp.float32)
    all_kv = lax.all_gather(own_kv, "seq", axis=1, tiled=True)

    def run_sweep(step_fn, init):
        return sweep(step_fn, init, all_kv, 0, positions)

    def stats_step(states, block_kv, key_pos):
        top, norm = states
        scores, visible = attend_block(query_rows, query_pos, block_kv, key_pos, scale)
        new_top = jnp.maximum(top, jnp.max(scores, axis=1, keepdims=True))
        weights = jnp.where(visible, jnp.exp(scores - new_top), 0.0)
        norm = jnp.exp(top - new_top) * norm + jnp.sum(weights, axis=1, keepdims=True)
        return (new_top, norm)

    top, norm = run_sweep(stats_step, (lowest_col, zeros_col))

    def block_probs(block_kv, key_pos):
        scores, visible = attend_block(query_rows, query_pos, block_kv, key_pos, scale)
        return jnp.where(visible, jnp.exp(scores - top), 0.0) / norm

    def out_step(acc_out, block_kv, key_pos):
        probs = block_probs(block_kv, key_pos)
        return acc_out + jnp.dot(
            probs.astype(jnp.bfloat16), block_kv[1], preferred_element_type=jnp.float32
        )

    attn_full = run_sweep(out_step, zeros_rows)
    delta = jnp.sum(d_attn.astype(jnp.float32) * attn_full, axis=1, keepdims=True)

    def grad_step(acc_grad, block_kv, key_pos):
        probs = block_probs(block_kv, key_pos)
        dprob = lax.dot_general(
            d_attn, block_kv[1], (((1,), (1,)), ((), ())), preferred_element_type=jnp.float32
        )
        dscore = (probs * (dprob - delta)).astype(jnp.bfloat16)
        return acc_grad + jnp.dot(dscore, block_kv[0], preferred_element_type=jnp.float32)

    d_rows = run_sweep(grad_step, zeros_rows) * scale
    attn = attn_full.astype(jnp.bfloat16).reshape(token_count, head_count, HD)
    d_query = d_rows.astype(jnp.bfloat16).reshape(token_count, head_count * HD)
    d_out_weight = lax.psum_scatter(
        jnp.einsum("td,thc->dhc", out_grad, attn, preferred_element_type=jnp.float32),
        "seq",
        scatter_dimension=0,
        tiled=True,
    )
    return (d_query, d_out_weight)


bf16, f32 = jnp.bfloat16, jnp.float32
ROWS = (((1,), (1,)), ((), ()))
COLS = (((0,), (0,)), ((), ()))


def dot(left, right, dims=(((1,), (0,)), ((), ()))):
    return lax.dot_general(left, right, dims, preferred_element_type=f32)


def xor_pairs(size, mask):
    return [(index, index ^ mask) for index in range(size)]


def vmem_call(kernel, outs, flops, *args):
    return pl.pallas_call(
        kernel,
        out_shape=[pltpu.VMEM(shape, dtype) for shape, dtype in outs],
        in_specs=[pl.BlockSpec(memory_space=pltpu.VMEM)] * len(args),
        out_specs=[pl.BlockSpec(memory_space=pltpu.VMEM)] * len(outs),
        cost_estimate=pl.CostEstimate(flops=flops, bytes_accessed=1 << 16, transcendentals=0),
    )(*args)


def pack_kernel(kv_ref, query_ref, out_ref):
    out_ref[:, :HD] = kv_ref[0]
    out_ref[:, HD : 2 * HD] = kv_ref[1]
    out_ref[:, 2 * HD :] = query_ref[...]


def slice_kernel(grad_ref, *out_refs):
    pair = lax.axis_index("seq") // 2
    span = out_refs[0].shape[1]
    for mask, out_ref in enumerate(out_refs):
        start = pl.multiple_of((pair ^ mask) * span, 128)
        out_ref[...] = grad_ref[:, pl.ds(start, span)]


def parts_kernel(grad_ref, weight_ref, own_ref, *rest):
    out_refs, flat = rest[:-1], rest[-1]
    rows, heads, _ = weight_ref.shape
    head = lax.axis_index("head")
    flat[...] = weight_ref[...].reshape(rows * heads, HD).astype(f32)
    cols = grad_ref[:, pl.ds(pl.multiple_of(head * rows, 128), rows)]
    per = own_ref.shape[1] // HD
    for mask, out_ref in enumerate((own_ref, *out_refs)):
        for h in range(per):
            weight = flat[pl.ds((head ^ mask) * per + h, rows, stride=heads), :].astype(bf16)
            out_ref[:, h * HD : (h + 1) * HD] = dot(cols, weight).astype(out_ref.dtype)


def join_kernel(*refs):
    token_refs, out_ref = refs[:-1], refs[-1]
    rows = token_refs[0].shape[0]
    for block, ref in enumerate(token_refs):
        out_ref[block * rows : (block + 1) * rows, :] = ref[:, : 2 * HD]


def attention_kernel(pos_ref, near_ref, far_ref, *refs):
    token_refs, (attn_ref, full_ref, prob_ref) = refs[:-3], refs[-3:]
    rows = token_refs[0].shape[0]
    blocks = len(token_refs)
    seq = lax.axis_index("seq")
    pair, low = seq // 2, seq % 2
    places = [
        pos_ref[pl.ds(2 * (pair ^ mask) + side, 1), :]
        for side in (low, 1 - low)
        for mask in range(blocks)
    ]
    key_pos = jnp.concatenate(places, axis=1)
    row_id = lax.broadcasted_iota(jnp.int32, (rows, rows), 0)
    col_id = lax.broadcasted_iota(jnp.int32, (rows, rows), 1)
    keys = jnp.concatenate([near_ref[:, :HD], far_ref[:, :HD]], axis=0)
    values = jnp.concatenate([near_ref[:, HD:], far_ref[:, HD:]], axis=0)
    scale = HD ** (-0.5)
    for block, ref in enumerate(token_refs):
        query_pos = jnp.sum(jnp.where(row_id == col_id, places[block], 0), axis=1, keepdims=True)
        visible = key_pos <= query_pos
        for h in range(full_ref.shape[1] // HD):
            scores = dot(ref[:, (2 + h) * HD : (3 + h) * HD], keys, ROWS) * scale
            scores = jnp.where(visible, scores, big_negative)
            top = jnp.max(scores, axis=1, keepdims=True)
            weights = jnp.exp(scores - top)
            share = 1.0 / jnp.sum(weights, axis=1, keepdims=True)
            full = dot(weights.astype(bf16), values) * share
            attn_ref[block * rows : (block + 1) * rows, h * HD : (h + 1) * HD] = full.astype(bf16)
            if block == 0:
                full_ref[:, h * HD : (h + 1) * HD] = full
                prob_ref[h] = weights * share


def query_kernel(near_ref, far_ref, full_ref, prob_ref, own_ref, *refs):
    part_refs, out_ref = refs[:-1], refs[-1]
    total = own_ref[...]
    for ref in part_refs:
        total = total + ref[...].astype(f32)
    d_attn = total.astype(bf16)
    half = near_ref.shape[0]
    for h in range(prob_ref.shape[0]):
        cols = slice(h * HD, (h + 1) * HD)
        grad = d_attn[:, cols]
        delta = jnp.sum(grad.astype(f32) * full_ref[:, cols], axis=1, keepdims=True)
        acc = 0.0
        for side, ref in enumerate((near_ref, far_ref)):
            dprob = dot(grad, ref[:, HD:], ROWS)
            prob = prob_ref[h, :, side * half : (side + 1) * half]
            acc = acc + dot((prob * (dprob - delta)).astype(bf16), ref[:, :HD])
        out_ref[:, cols] = (acc * HD ** (-0.5)).astype(bf16)


def sums_kernel(attn_ref, *refs):
    grad_refs, (mine_ref, theirs_ref) = refs[:-2], refs[-2:]
    low = lax.axis_index("seq") % 2
    grads = jnp.concatenate([ref[...] for ref in grad_refs], axis=0)
    sums = dot(grads, attn_ref[...], COLS)
    half = sums.shape[0] // 2
    mine_ref[pl.ds(0, half), :] = jnp.where(low == 0, sums[:half], sums[half:])
    theirs_ref[pl.ds(0, half), :] = jnp.where(low == 0, sums[half:], sums[:half])


def add_kernel(mine_ref, theirs_ref, out_ref):
    for h in range(out_ref.shape[1]):
        cols = slice(h * HD, (h + 1) * HD)
        out_ref[:, h, :] = mine_ref[:, cols] + theirs_ref[:, cols]


def narrow_body(queries, keys_values, out_weight, out_grad, positions, seq_size, head_size):
    token_count = queries.shape[0]
    head_count = queries.shape[1] // HD
    width = head_count * HD
    head_index = lax.axis_index("head")
    pair_count = seq_size // 2
    span = out_grad.shape[1] // pair_count
    rows_in = out_weight.shape[0]
    tokens_near = pair_count * token_count
    if keys_values.shape[2] == HD:
        own_kv = keys_values
    else:
        own_kv = lax.dynamic_slice_in_dim(keys_values, head_index * head_count // GROUP * HD, HD, 2)

    def move(array, axis, size, mask):
        return lax.ppermute(array, axis, xor_pairs(size, mask))

    masks = range(1, pair_count)
    (own_tokens,) = vmem_call(
        pack_kernel, [((token_count, 2 * HD + width), bf16)], 1 << 20, own_kv, queries
    )
    tokens = [own_tokens] + [move(own_tokens, "seq", seq_size, 2 * m) for m in masks]
    grads = vmem_call(slice_kernel, [((token_count, span), bf16)] * pair_count, 1 << 20, out_grad)
    grads = [grads[0]] + [move(grads[m], "seq", seq_size, 2 * m) for m in masks]

    kinds = [f32] + [bf16] * (head_size - 1)
    parts = pl.pallas_call(
        parts_kernel,
        out_shape=[pltpu.VMEM((token_count, width), kind) for kind in kinds],
        in_specs=[pl.BlockSpec(memory_space=pltpu.VMEM)] * 2,
        out_specs=[pl.BlockSpec(memory_space=pltpu.VMEM)] * head_size,
        scratch_shapes=[pltpu.VMEM((rows_in * out_weight.shape[1], HD), f32)],
        cost_estimate=pl.CostEstimate(flops=1 << 28, bytes_accessed=1 << 20, transcendentals=0),
    )(out_grad, out_weight)
    parts = [parts[0]] + [move(parts[m], "head", head_size, m) for m in range(1, head_size)]

    (near,) = vmem_call(join_kernel, [((tokens_near, 2 * HD), bf16)], 1 << 20, *tokens)
    far = move(near, "seq", seq_size, 1)
    attn, full, prob = vmem_call(
        attention_kernel,
        [
            ((tokens_near, width), bf16),
            ((token_count, width), f32),
            ((head_count, token_count, 2 * tokens_near), f32),
        ],
        1 << 29,
        positions.reshape(seq_size, token_count),
        near,
        far,
        *tokens,
    )
    mine, theirs = vmem_call(sums_kernel, [((span // 2, width), f32)] * 2, 1 << 28, attn, *grads)
    theirs = move(theirs, "seq", seq_size, 1)
    d_query = pl.pallas_call(
        query_kernel,
        out_shape=jax.ShapeDtypeStruct((token_count, width), bf16),
        cost_estimate=pl.CostEstimate(flops=1 << 28, bytes_accessed=1 << 20, transcendentals=0),
    )(near, far, full, prob, *parts)
    d_out_weight = pl.pallas_call(
        add_kernel,
        out_shape=jax.ShapeDtypeStruct((span // 2, head_count, HD), f32),
        cost_estimate=pl.CostEstimate(flops=1 << 20, bytes_accessed=1 << 20, transcendentals=0),
    )(mine, theirs)
    return (d_query, d_out_weight)


def solution(mesh):
    seq_size, head_size = mesh.shape["seq"], mesh.shape["head"]
    narrow = seq_size in (4, 8) and head_size in (2, 4, 8)

    def body(*arrays):
        if not narrow:
            return wide_body(*arrays)
        return narrow_body(*arrays, seq_size, head_size)

    return jax.shard_map(
        body,
        mesh=mesh,
        in_specs=(
            P("seq", "head"),
            P(None, "seq", None),
            P("head", None, None),
            P("seq", None),
            P(),
        ),
        out_specs=(P("seq", "head"), P("seq", "head", None)),
        check_vma=False,
    )
```

```python
import math

import jax
import jax.numpy as jnp
from jax import lax
from jax.experimental import pallas as pl
from jax.experimental.pallas import tpu as pltpu
from jax.sharding import PartitionSpec as P


HD = 128
GROUP = 8


big_negative = -1e30


def attend_block(query_rows, query_pos, block_kv, key_pos, scale):
    scores = (
        lax.dot_general(
            query_rows, block_kv[0], (((1,), (1,)), ((), ())), preferred_element_type=jnp.float32
        )
        * scale
    )
    visible = key_pos[None, :] <= query_pos[:, None]
    return (jnp.where(visible, scores, big_negative), visible)


def sweep(step_fn, states, key_piece, offset, positions):
    span_size = key_piece.shape[1]
    block_size = math.gcd(span_size, 1024)

    def step(step_index, inner):
        block_kv = lax.dynamic_slice_in_dim(key_piece, step_index * block_size, block_size, 1)
        key_pos = lax.dynamic_slice_in_dim(
            positions, offset + step_index * block_size, block_size, 0
        )
        return step_fn(inner, block_kv, key_pos)

    return lax.fori_loop(0, span_size // block_size, step, states)


def wide_body(queries, keys_values, out_weight, out_grad, positions):
    token_count = queries.shape[0]
    head_count = queries.shape[1] // HD
    scale = HD ** (-0.5)
    seq_index = lax.axis_index("seq")
    head_index = lax.axis_index("head")
    kv_group = head_index * head_count // GROUP
    own_kv = lax.dynamic_slice_in_dim(keys_values, kv_group * HD, HD, 2)
    own_pos = lax.dynamic_slice_in_dim(positions, seq_index * token_count, token_count, 0)
    query_pos = jnp.repeat(own_pos, head_count)
    query_rows = queries.reshape(token_count * head_count, HD)
    d_attn = jnp.einsum(
        "td,dhc->thc",
        out_grad,
        lax.all_to_all(out_weight, "head", split_axis=1, concat_axis=0, tiled=True),
        preferred_element_type=jnp.float32,
    )
    d_attn = d_attn.astype(jnp.bfloat16).reshape(token_count * head_count, HD)
    row_total = token_count * head_count
    zeros_col = jnp.zeros((row_total, 1), jnp.float32)
    zeros_rows = jnp.zeros((row_total, HD), jnp.float32)
    lowest_col = jnp.full((row_total, 1), big_negative, jnp.float32)
    all_kv = lax.all_gather(own_kv, "seq", axis=1, tiled=True)

    def run_sweep(step_fn, init):
        return sweep(step_fn, init, all_kv, 0, positions)

    def stats_step(states, block_kv, key_pos):
        top, norm = states
        scores, visible = attend_block(query_rows, query_pos, block_kv, key_pos, scale)
        new_top = jnp.maximum(top, jnp.max(scores, axis=1, keepdims=True))
        weights = jnp.where(visible, jnp.exp(scores - new_top), 0.0)
        norm = jnp.exp(top - new_top) * norm + jnp.sum(weights, axis=1, keepdims=True)
        return (new_top, norm)

    top, norm = run_sweep(stats_step, (lowest_col, zeros_col))

    def block_probs(block_kv, key_pos):
        scores, visible = attend_block(query_rows, query_pos, block_kv, key_pos, scale)
        return jnp.where(visible, jnp.exp(scores - top), 0.0) / norm

    def out_step(acc_out, block_kv, key_pos):
        probs = block_probs(block_kv, key_pos)
        return acc_out + jnp.dot(
            probs.astype(jnp.bfloat16), block_kv[1], preferred_element_type=jnp.float32
        )

    attn_full = run_sweep(out_step, zeros_rows)
    delta = jnp.sum(d_attn.astype(jnp.float32) * attn_full, axis=1, keepdims=True)

    def grad_step(acc_grad, block_kv, key_pos):
        probs = block_probs(block_kv, key_pos)
        dprob = lax.dot_general(
            d_attn, block_kv[1], (((1,), (1,)), ((), ())), preferred_element_type=jnp.float32
        )
        dscore = (probs * (dprob - delta)).astype(jnp.bfloat16)
        return acc_grad + jnp.dot(dscore, block_kv[0], preferred_element_type=jnp.float32)

    d_rows = run_sweep(grad_step, zeros_rows) * scale
    attn = attn_full.astype(jnp.bfloat16).reshape(token_count, head_count, HD)
    d_query = d_rows.astype(jnp.bfloat16).reshape(token_count, head_count * HD)
    d_out_weight = lax.psum_scatter(
        jnp.einsum("td,thc->dhc", out_grad, attn, preferred_element_type=jnp.float32),
        "seq",
        scatter_dimension=0,
        tiled=True,
    )
    return (d_query, d_out_weight)


bf16, f32 = jnp.bfloat16, jnp.float32
ROWS = (((1,), (1,)), ((), ()))
COLS = (((0,), (0,)), ((), ()))


def dot(left, right, dims=(((1,), (0,)), ((), ()))):
    return lax.dot_general(left, right, dims, preferred_element_type=f32)


def xor_pairs(size, mask):
    return [(index, index ^ mask) for index in range(size)]


def vmem_call(kernel, outs, flops, limit, *args):
    return pl.pallas_call(
        kernel,
        out_shape=[pltpu.VMEM(shape, dtype) for shape, dtype in outs],
        in_specs=[pl.BlockSpec(memory_space=pltpu.VMEM)] * len(args),
        out_specs=[pl.BlockSpec(memory_space=pltpu.VMEM)] * len(outs),
        cost_estimate=pl.CostEstimate(flops=flops, bytes_accessed=1 << 16, transcendentals=0),
        compiler_params=pltpu.CompilerParams(vmem_limit_bytes=limit << 20),
    )(*args)


def pack_kernel(kv_ref, query_ref, out_ref, sems):
    copies = [
        pltpu.make_async_copy(source, out_ref.at[:, cols], sems.at[index])
        for index, (source, cols) in enumerate(
            (
                (kv_ref.at[0], slice(0, HD)),
                (kv_ref.at[1], slice(HD, 2 * HD)),
                (query_ref, slice(2 * HD, out_ref.shape[1])),
            )
        )
    ]
    for copy in copies:
        copy.start()
    for copy in copies:
        copy.wait()


def slice_kernel(grad_ref, *out_refs):
    pair = lax.axis_index("seq") // 2
    span = out_refs[0].shape[1]
    for mask, out_ref in enumerate(out_refs):
        start = pl.multiple_of((pair ^ mask) * span, 128)
        out_ref[...] = grad_ref[:, pl.ds(start, span)]


def parts_kernel(grad_ref, weight_ref, own_ref, *rest):
    out_refs, flat = rest[:-1], rest[-1]
    rows, heads, _ = weight_ref.shape
    head = lax.axis_index("head")
    flat[...] = weight_ref[...].reshape(rows * heads, HD).astype(f32)
    cols = grad_ref[:, pl.ds(pl.multiple_of(head * rows, 128), rows)]
    per = own_ref.shape[1] // HD
    for mask, out_ref in enumerate((own_ref, *out_refs)):
        for h in range(per):
            weight = flat[pl.ds((head ^ mask) * per + h, rows, stride=heads), :].astype(bf16)
            out_ref[:, h * HD : (h + 1) * HD] = dot(cols, weight).astype(out_ref.dtype)


def join_kernel(*refs):
    token_refs, out_ref = refs[:-1], refs[-1]
    rows = token_refs[0].shape[0]
    for block, ref in enumerate(token_refs):
        out_ref[block * rows : (block + 1) * rows, :] = ref[:, : 2 * HD]


def attention_kernel(pos_ref, near_ref, far_ref, *refs):
    token_refs, (attn_ref, full_ref, prob_ref) = refs[:-3], refs[-3:]
    rows = token_refs[0].shape[0]
    blocks = len(token_refs)
    seq = lax.axis_index("seq")
    pair, low = seq // 2, seq % 2
    places = [
        pos_ref[pl.ds(2 * (pair ^ mask) + side, 1), :]
        for side in (low, 1 - low)
        for mask in range(blocks)
    ]
    key_pos = jnp.concatenate(places, axis=1)
    row_id = lax.broadcasted_iota(jnp.int32, (rows, rows), 0)
    col_id = lax.broadcasted_iota(jnp.int32, (rows, rows), 1)
    keys = jnp.concatenate([near_ref[:, :HD], far_ref[:, :HD]], axis=0)
    values = jnp.concatenate([near_ref[:, HD:], far_ref[:, HD:]], axis=0)
    scale = HD ** (-0.5)
    for block, ref in enumerate(token_refs):
        query_pos = jnp.sum(jnp.where(row_id == col_id, places[block], 0), axis=1, keepdims=True)
        visible = key_pos <= query_pos
        for h in range(full_ref.shape[1] // HD):
            scores = dot(ref[:, (2 + h) * HD : (3 + h) * HD], keys, ROWS) * scale
            scores = jnp.where(visible, scores, big_negative)
            top = jnp.max(scores, axis=1, keepdims=True)
            weights = jnp.exp(scores - top)
            share = 1.0 / jnp.sum(weights, axis=1, keepdims=True)
            full = dot(weights.astype(bf16), values) * share
            attn_ref[block * rows : (block + 1) * rows, h * HD : (h + 1) * HD] = full.astype(bf16)
            if block == 0:
                full_ref[:, h * HD : (h + 1) * HD] = full
                prob_ref[h] = weights * share


def query_kernel(near_ref, far_ref, full_ref, prob_ref, own_ref, *refs):
    part_refs, out_ref = refs[:-1], refs[-1]
    total = own_ref[...]
    for ref in part_refs:
        total = total + ref[...].astype(f32)
    d_attn = total.astype(bf16)
    half = near_ref.shape[0]
    for h in range(prob_ref.shape[0]):
        cols = slice(h * HD, (h + 1) * HD)
        grad = d_attn[:, cols]
        delta = jnp.sum(grad.astype(f32) * full_ref[:, cols], axis=1, keepdims=True)
        acc = 0.0
        for side, ref in enumerate((near_ref, far_ref)):
            dprob = dot(grad, ref[:, HD:], ROWS)
            prob = prob_ref[h, :, side * half : (side + 1) * half]
            acc = acc + dot((prob * (dprob - delta)).astype(bf16), ref[:, :HD])
        out_ref[:, cols] = (acc * HD ** (-0.5)).astype(bf16)


def sums_kernel(attn_ref, *refs):
    grad_refs, (mine_ref, theirs_ref) = refs[:-2], refs[-2:]
    low = lax.axis_index("seq") % 2
    grads = jnp.concatenate([ref[...] for ref in grad_refs], axis=0)
    sums = dot(grads, attn_ref[...], COLS)
    half = sums.shape[0] // 2
    mine_ref[pl.ds(0, half), :] = jnp.where(low == 0, sums[:half], sums[half:])
    theirs_ref[pl.ds(0, half), :] = jnp.where(low == 0, sums[half:], sums[:half])


def add_kernel(mine_ref, theirs_ref, out_ref):
    for h in range(out_ref.shape[1]):
        cols = slice(h * HD, (h + 1) * HD)
        out_ref[:, h, :] = mine_ref[:, cols] + theirs_ref[:, cols]


def narrow_body(queries, keys_values, out_weight, out_grad, positions, seq_size, head_size):
    token_count = queries.shape[0]
    head_count = queries.shape[1] // HD
    width = head_count * HD
    head_index = lax.axis_index("head")
    pair_count = seq_size // 2
    span = out_grad.shape[1] // pair_count
    rows_in = out_weight.shape[0]
    tokens_near = pair_count * token_count
    if keys_values.shape[2] == HD:
        own_kv = keys_values
    else:
        own_kv = lax.dynamic_slice_in_dim(keys_values, head_index * head_count // GROUP * HD, HD, 2)

    def move(array, axis, size, mask):
        return lax.ppermute(array, axis, xor_pairs(size, mask))

    masks = range(1, pair_count)
    own_tokens = pl.pallas_call(
        pack_kernel,
        out_shape=pltpu.VMEM((token_count, 2 * HD + width), bf16),
        in_specs=[pl.BlockSpec(memory_space=pltpu.HBM)] * 2,
        out_specs=pl.BlockSpec(memory_space=pltpu.VMEM),
        scratch_shapes=[pltpu.SemaphoreType.DMA((3,))],
        cost_estimate=pl.CostEstimate(flops=1 << 32, bytes_accessed=1 << 18, transcendentals=0),
        compiler_params=pltpu.CompilerParams(vmem_limit_bytes=2 << 20),
    )(
        pltpu.with_memory_space_constraint(own_kv, pltpu.HBM),
        pltpu.with_memory_space_constraint(queries, pltpu.HBM),
    )
    tokens = [own_tokens] + [move(own_tokens, "seq", seq_size, 2 * m) for m in masks]
    grads = vmem_call(
        slice_kernel, [((token_count, span), bf16)] * pair_count, 1 << 32, 4, out_grad
    )
    grads = [grads[0]] + [move(grads[m], "seq", seq_size, 2 * m) for m in masks]

    kinds = [f32] + [bf16] * (head_size - 1)
    parts = pl.pallas_call(
        parts_kernel,
        out_shape=[pltpu.VMEM((token_count, width), kind) for kind in kinds],
        in_specs=[pl.BlockSpec(memory_space=pltpu.VMEM)] * 2,
        out_specs=[pl.BlockSpec(memory_space=pltpu.VMEM)] * head_size,
        scratch_shapes=[pltpu.VMEM((rows_in * out_weight.shape[1], HD), f32)],
        cost_estimate=pl.CostEstimate(flops=1 << 28, bytes_accessed=1 << 20, transcendentals=0),
        compiler_params=pltpu.CompilerParams(vmem_limit_bytes=16 << 20),
    )(out_grad, out_weight)
    parts = [parts[0]] + [move(parts[m], "head", head_size, m) for m in range(1, head_size)]

    (near,) = vmem_call(join_kernel, [((tokens_near, 2 * HD), bf16)], 1 << 20, 2, *tokens)
    far = move(near, "seq", seq_size, 1)
    attn, full, prob = vmem_call(
        attention_kernel,
        [
            ((tokens_near, width), bf16),
            ((token_count, width), f32),
            ((head_count, token_count, 2 * tokens_near), f32),
        ],
        1 << 29,
        24,
        positions.reshape(seq_size, token_count),
        near,
        far,
        *tokens,
    )
    mine, theirs = vmem_call(
        sums_kernel, [((span // 2, width), f32)] * 2, 1 << 28, 12, attn, *grads
    )
    theirs = move(theirs, "seq", seq_size, 1)
    d_query = pl.pallas_call(
        query_kernel,
        out_shape=jax.ShapeDtypeStruct((token_count, width), bf16),
        cost_estimate=pl.CostEstimate(flops=1 << 28, bytes_accessed=1 << 20, transcendentals=0),
        compiler_params=pltpu.CompilerParams(vmem_limit_bytes=8 << 20),
    )(near, far, full, prob, *parts)
    d_out_weight = pl.pallas_call(
        add_kernel,
        out_shape=jax.ShapeDtypeStruct((span // 2, head_count, HD), f32),
        cost_estimate=pl.CostEstimate(flops=1 << 20, bytes_accessed=1 << 20, transcendentals=0),
        compiler_params=pltpu.CompilerParams(vmem_limit_bytes=4 << 20),
    )(mine, theirs)
    return (d_query, d_out_weight)


def solution(mesh):
    seq_size, head_size = mesh.shape["seq"], mesh.shape["head"]
    narrow = seq_size in (4, 8) and head_size in (2, 4, 8)

    def body(*arrays):
        if not narrow:
            return wide_body(*arrays)
        return narrow_body(*arrays, seq_size, head_size)

    return jax.shard_map(
        body,
        mesh=mesh,
        in_specs=(
            P("seq", "head"),
            P(None, "seq", None),
            P("head", None, None),
            P("seq", None),
            P(),
        ),
        out_specs=(P("seq", "head"), P("seq", "head", None)),
        check_vma=False,
    )
```

```python
import functools
import math

import jax
import jax.numpy as jnp
from jax import lax
from jax.experimental import pallas as pl
from jax.experimental.pallas import tpu as pltpu
from jax.sharding import PartitionSpec as P


HD = 128
GROUP = 8


big_negative = -1e30


def attend_block(query_rows, query_pos, block_kv, key_pos, scale):
    scores = (
        lax.dot_general(
            query_rows, block_kv[0], (((1,), (1,)), ((), ())), preferred_element_type=jnp.float32
        )
        * scale
    )
    visible = key_pos[None, :] <= query_pos[:, None]
    return (jnp.where(visible, scores, big_negative), visible)


def sweep(step_fn, states, key_piece, offset, positions):
    span_size = key_piece.shape[1]
    block_size = math.gcd(span_size, 1024)

    def step(step_index, inner):
        block_kv = lax.dynamic_slice_in_dim(key_piece, step_index * block_size, block_size, 1)
        key_pos = lax.dynamic_slice_in_dim(
            positions, offset + step_index * block_size, block_size, 0
        )
        return step_fn(inner, block_kv, key_pos)

    return lax.fori_loop(0, span_size // block_size, step, states)


def wide_body(queries, keys_values, out_weight, out_grad, positions):
    token_count = queries.shape[0]
    head_count = queries.shape[1] // HD
    scale = HD ** (-0.5)
    seq_index = lax.axis_index("seq")
    head_index = lax.axis_index("head")
    kv_group = head_index * head_count // GROUP
    own_kv = lax.dynamic_slice_in_dim(keys_values, kv_group * HD, HD, 2)
    own_pos = lax.dynamic_slice_in_dim(positions, seq_index * token_count, token_count, 0)
    query_pos = jnp.repeat(own_pos, head_count)
    query_rows = queries.reshape(token_count * head_count, HD)
    d_attn = jnp.einsum(
        "td,dhc->thc",
        out_grad,
        lax.all_to_all(out_weight, "head", split_axis=1, concat_axis=0, tiled=True),
        preferred_element_type=jnp.float32,
    )
    d_attn = d_attn.astype(jnp.bfloat16).reshape(token_count * head_count, HD)
    row_total = token_count * head_count
    zeros_col = jnp.zeros((row_total, 1), jnp.float32)
    zeros_rows = jnp.zeros((row_total, HD), jnp.float32)
    lowest_col = jnp.full((row_total, 1), big_negative, jnp.float32)
    all_kv = lax.all_gather(own_kv, "seq", axis=1, tiled=True)

    def run_sweep(step_fn, init):
        return sweep(step_fn, init, all_kv, 0, positions)

    def stats_step(states, block_kv, key_pos):
        top, norm = states
        scores, visible = attend_block(query_rows, query_pos, block_kv, key_pos, scale)
        new_top = jnp.maximum(top, jnp.max(scores, axis=1, keepdims=True))
        weights = jnp.where(visible, jnp.exp(scores - new_top), 0.0)
        norm = jnp.exp(top - new_top) * norm + jnp.sum(weights, axis=1, keepdims=True)
        return (new_top, norm)

    top, norm = run_sweep(stats_step, (lowest_col, zeros_col))

    def block_probs(block_kv, key_pos):
        scores, visible = attend_block(query_rows, query_pos, block_kv, key_pos, scale)
        return jnp.where(visible, jnp.exp(scores - top), 0.0) / norm

    def out_step(acc_out, block_kv, key_pos):
        probs = block_probs(block_kv, key_pos)
        return acc_out + jnp.dot(
            probs.astype(jnp.bfloat16), block_kv[1], preferred_element_type=jnp.float32
        )

    attn_full = run_sweep(out_step, zeros_rows)
    delta = jnp.sum(d_attn.astype(jnp.float32) * attn_full, axis=1, keepdims=True)

    def grad_step(acc_grad, block_kv, key_pos):
        probs = block_probs(block_kv, key_pos)
        dprob = lax.dot_general(
            d_attn, block_kv[1], (((1,), (1,)), ((), ())), preferred_element_type=jnp.float32
        )
        dscore = (probs * (dprob - delta)).astype(jnp.bfloat16)
        return acc_grad + jnp.dot(dscore, block_kv[0], preferred_element_type=jnp.float32)

    d_rows = run_sweep(grad_step, zeros_rows) * scale
    attn = attn_full.astype(jnp.bfloat16).reshape(token_count, head_count, HD)
    d_query = d_rows.astype(jnp.bfloat16).reshape(token_count, head_count * HD)
    d_out_weight = lax.psum_scatter(
        jnp.einsum("td,thc->dhc", out_grad, attn, preferred_element_type=jnp.float32),
        "seq",
        scatter_dimension=0,
        tiled=True,
    )
    return (d_query, d_out_weight)


bf16, f32 = jnp.bfloat16, jnp.float32
ROWS = (((1,), (1,)), ((), ()))
COLS = (((0,), (0,)), ((), ()))


def dot(left, right, dims=(((1,), (0,)), ((), ()))):
    return lax.dot_general(left, right, dims, preferred_element_type=f32)


def xor_pairs(size, mask):
    return [(index, index ^ mask) for index in range(size)]


def vmem_call(kernel, outs, flops, limit, *args, scratch=()):
    return pl.pallas_call(
        kernel,
        out_shape=[pltpu.VMEM(shape, dtype) for shape, dtype in outs],
        in_specs=[pl.BlockSpec(memory_space=pltpu.VMEM)] * len(args),
        out_specs=[pl.BlockSpec(memory_space=pltpu.VMEM)] * len(outs),
        scratch_shapes=[pltpu.VMEM(shape, dtype) for shape, dtype in scratch],
        cost_estimate=pl.CostEstimate(flops=flops, bytes_accessed=1 << 16, transcendentals=0),
        compiler_params=pltpu.CompilerParams(vmem_limit_bytes=limit << 20),
    )(*args)


def pack_kernel(kv_ref, query_ref, out_ref, sems):
    copies = [
        pltpu.make_async_copy(source, out_ref.at[:, cols], sems.at[index])
        for index, (source, cols) in enumerate(
            (
                (kv_ref.at[0], slice(0, HD)),
                (kv_ref.at[1], slice(HD, 2 * HD)),
                (query_ref, slice(2 * HD, out_ref.shape[1])),
            )
        )
    ]
    for copy in copies:
        copy.start()
    for copy in copies:
        copy.wait()


def slice_kernel(grad_ref, *out_refs):
    pair = lax.axis_index("seq") // 2
    span = out_refs[0].shape[1]
    for mask, out_ref in enumerate(out_refs):
        start = pl.multiple_of((pair ^ mask) * span, 128)
        out_ref[...] = grad_ref[:, pl.ds(start, span)]


def split_masks(masks, bit):
    kept = [mask for mask in masks if not mask & bit]
    return kept, [mask | bit for mask in kept]


def parts_kernel(grad_ref, weight_ref, kept_ref, sent_ref, flat):
    rows, heads, _ = weight_ref.shape
    head = lax.axis_index("head")
    flat[...] = weight_ref[...].reshape(rows * heads, HD).astype(f32)
    cols = grad_ref[:, pl.ds(pl.multiple_of(head * rows, 128), rows)]
    size = lax.axis_size("head")
    per = heads // size
    for out_ref, masks in zip((kept_ref, sent_ref), split_masks(range(size), 1)):
        for place, mask in enumerate(masks):
            for h in range(per):
                weight = flat[pl.ds((head ^ mask) * per + h, rows, stride=heads), :].astype(bf16)
                start = (place * per + h) * HD
                out_ref[:, start : start + HD] = dot(cols, weight).astype(out_ref.dtype)


def blend_kernel(width, bit, kept_ref, got_ref, next_ref, sent_ref):
    masks = [mask for mask in range(lax.axis_size("head")) if not mask & (bit - 1)]
    for out_ref, chosen in zip((next_ref, sent_ref), split_masks(masks, bit)):
        for place, mask in enumerate(chosen):
            cols = slice(masks.index(mask) * width, (masks.index(mask) + 1) * width)
            total = kept_ref[:, cols] + got_ref[:, cols].astype(f32)
            out_ref[:, place * width : (place + 1) * width] = total.astype(out_ref.dtype)


def join_kernel(*refs):
    token_refs, out_ref = refs[:-1], refs[-1]
    rows = token_refs[0].shape[0]
    for block, ref in enumerate(token_refs):
        out_ref[block * rows : (block + 1) * rows, :] = ref[:, : 2 * HD]


def attention_kernel(pos_ref, near_ref, far_ref, *refs):
    token_refs, (attn_ref, full_ref, prob_ref, score_ref, weight_ref) = refs[:-5], refs[-5:]
    rows = token_refs[0].shape[0]
    blocks = len(token_refs)
    half = blocks * rows
    seq = lax.axis_index("seq")
    pair, low = seq // 2, seq % 2
    places = [
        pos_ref[pl.ds(2 * (pair ^ mask) + side, 1), :]
        for side in (low, 1 - low)
        for mask in range(blocks)
    ]
    key_pos = jnp.concatenate(places, axis=1)
    row_id = lax.broadcasted_iota(jnp.int32, (rows, rows), 0)
    col_id = lax.broadcasted_iota(jnp.int32, (rows, rows), 1)
    heads = range(score_ref.shape[0])
    for h in heads:
        query = jnp.concatenate([ref[:, (2 + h) * HD : (3 + h) * HD] for ref in token_refs], axis=0)
        score_ref[h, :, :half] = dot(query, near_ref[:, :HD], ROWS)
        score_ref[h, :, half:] = dot(query, far_ref[:, :HD], ROWS)
    for h in heads:
        cols = slice(h * HD, (h + 1) * HD)
        shares = []
        for block in range(blocks):
            span = slice(block * rows, (block + 1) * rows)
            query_pos = jnp.sum(
                jnp.where(row_id == col_id, places[block], 0), axis=1, keepdims=True
            )
            scores = jnp.where(key_pos <= query_pos, score_ref[h, span, :], big_negative)
            top = jnp.max(scores, axis=1, keepdims=True)
            weights = jnp.exp2((scores - top) * (HD ** (-0.5) * math.log2(math.e)))
            shares.append(1.0 / jnp.sum(weights, axis=1, keepdims=True))
            weight_ref[h, span, :] = weights.astype(bf16)
            if block == 0:
                prob_ref[h] = weights * shares[0]
        full = dot(weight_ref[h, :, :half], near_ref[:, HD:])
        full = full + dot(weight_ref[h, :, half:], far_ref[:, HD:])
        full = full * jnp.concatenate(shares, axis=0)
        attn_ref[:, cols] = full.astype(bf16)
        full_ref[:, cols] = full[:rows]


def query_kernel(near_ref, far_ref, full_ref, prob_ref, kept_ref, got_ref, out_ref):
    d_attn = (kept_ref[...] + got_ref[...].astype(f32)).astype(bf16)
    half = near_ref.shape[0]
    for h in range(prob_ref.shape[0]):
        cols = slice(h * HD, (h + 1) * HD)
        grad = d_attn[:, cols]
        delta = jnp.sum(grad.astype(f32) * full_ref[:, cols], axis=1, keepdims=True)
        acc = 0.0
        for side, ref in enumerate((near_ref, far_ref)):
            dprob = dot(grad, ref[:, HD:], ROWS)
            prob = prob_ref[h, :, side * half : (side + 1) * half]
            acc = acc + dot((prob * (dprob - delta)).astype(bf16), ref[:, :HD])
        out_ref[:, cols] = (acc * HD ** (-0.5)).astype(bf16)


def sums_kernel(attn_ref, *refs):
    grad_refs, (mine_ref, theirs_ref) = refs[:-2], refs[-2:]
    low = lax.axis_index("seq") % 2
    grads = jnp.concatenate([ref[...] for ref in grad_refs], axis=0)
    sums = dot(grads, attn_ref[...], COLS)
    half = sums.shape[0] // 2
    mine_ref[pl.ds(0, half), :] = jnp.where(low == 0, sums[:half], sums[half:])
    theirs_ref[pl.ds(0, half), :] = jnp.where(low == 0, sums[half:], sums[:half])


def add_kernel(mine_ref, theirs_ref, out_ref):
    for h in range(out_ref.shape[1]):
        cols = slice(h * HD, (h + 1) * HD)
        out_ref[:, h, :] = mine_ref[:, cols] + theirs_ref[:, cols]


def narrow_body(queries, keys_values, out_weight, out_grad, positions, seq_size, head_size):
    token_count = queries.shape[0]
    head_count = queries.shape[1] // HD
    width = head_count * HD
    head_index = lax.axis_index("head")
    pair_count = seq_size // 2
    span = out_grad.shape[1] // pair_count
    rows_in = out_weight.shape[0]
    tokens_near = pair_count * token_count
    if keys_values.shape[2] == HD:
        own_kv = keys_values
    else:
        own_kv = lax.dynamic_slice_in_dim(keys_values, head_index * head_count // GROUP * HD, HD, 2)

    def move(array, axis, size, mask):
        return lax.ppermute(array, axis, xor_pairs(size, mask))

    masks = range(1, pair_count)
    own_tokens = pl.pallas_call(
        pack_kernel,
        out_shape=pltpu.VMEM((token_count, 2 * HD + width), bf16),
        in_specs=[pl.BlockSpec(memory_space=pltpu.HBM)] * 2,
        out_specs=pl.BlockSpec(memory_space=pltpu.VMEM),
        scratch_shapes=[pltpu.SemaphoreType.DMA((3,))],
        cost_estimate=pl.CostEstimate(flops=1 << 32, bytes_accessed=1 << 18, transcendentals=0),
        compiler_params=pltpu.CompilerParams(vmem_limit_bytes=2 << 20),
    )(
        pltpu.with_memory_space_constraint(own_kv, pltpu.HBM),
        pltpu.with_memory_space_constraint(queries, pltpu.HBM),
    )
    tokens = [own_tokens] + [move(own_tokens, "seq", seq_size, 2 * m) for m in masks]
    grads = vmem_call(
        slice_kernel, [((token_count, span), bf16)] * pair_count, 1 << 32, 4, out_grad
    )
    grads = [grads[0]] + [move(grads[m], "seq", seq_size, 2 * m) for m in masks]

    half = (token_count, head_size // 2 * width)
    kept, sent = vmem_call(
        parts_kernel,
        [(half, f32), (half, bf16)],
        1 << 28,
        16,
        out_grad,
        out_weight,
        scratch=[((rows_in * out_weight.shape[1], HD), f32)],
    )
    got = move(sent, "head", head_size, 1)
    bit = 2
    while bit < head_size:
        half = (token_count, kept.shape[1] // 2)
        kept, sent = vmem_call(
            functools.partial(blend_kernel, width, bit),
            [(half, f32), (half, bf16)],
            1 << 20,
            2,
            kept,
            got,
        )
        got = move(sent, "head", head_size, bit)
        bit *= 2

    (near,) = vmem_call(join_kernel, [((tokens_near, 2 * HD), bf16)], 1 << 20, 2, *tokens)
    far = move(near, "seq", seq_size, 1)
    attn, full, prob = vmem_call(
        attention_kernel,
        [
            ((tokens_near, width), bf16),
            ((token_count, width), f32),
            ((head_count, token_count, 2 * tokens_near), f32),
        ],
        1 << 29,
        24,
        positions.reshape(seq_size, token_count),
        near,
        far,
        *tokens,
        scratch=[
            ((head_count, tokens_near, 2 * tokens_near), kind) for kind in (f32, bf16)
        ],
    )
    mine, theirs = vmem_call(
        sums_kernel, [((span // 2, width), f32)] * 2, 1 << 28, 12, attn, *grads
    )
    theirs = move(theirs, "seq", seq_size, 1)
    d_query = pl.pallas_call(
        query_kernel,
        out_shape=jax.ShapeDtypeStruct((token_count, width), bf16),
        cost_estimate=pl.CostEstimate(flops=1 << 28, bytes_accessed=1 << 20, transcendentals=0),
        compiler_params=pltpu.CompilerParams(vmem_limit_bytes=8 << 20),
    )(near, far, full, prob, kept, got)
    d_out_weight = pl.pallas_call(
        add_kernel,
        out_shape=jax.ShapeDtypeStruct((span // 2, head_count, HD), f32),
        cost_estimate=pl.CostEstimate(flops=1 << 20, bytes_accessed=1 << 20, transcendentals=0),
        compiler_params=pltpu.CompilerParams(vmem_limit_bytes=4 << 20),
    )(mine, theirs)
    return (d_query, d_out_weight)


def solution(mesh):
    seq_size, head_size = mesh.shape["seq"], mesh.shape["head"]
    narrow = seq_size in (4, 8) and head_size in (2, 4, 8)

    def body(*arrays):
        if not narrow:
            return wide_body(*arrays)
        return narrow_body(*arrays, seq_size, head_size)

    return jax.shard_map(
        body,
        mesh=mesh,
        in_specs=(
            P("seq", "head"),
            P(None, "seq", None),
            P("head", None, None),
            P("seq", None),
            P(),
        ),
        out_specs=(P("seq", "head"), P("seq", "head", None)),
        check_vma=False,
    )
```

```python
import functools
import math

import jax
import jax.numpy as jnp
from jax import lax
from jax.experimental import pallas as pl
from jax.experimental.pallas import tpu as pltpu
from jax.sharding import PartitionSpec as P


HD = 128
GROUP = 8


big_negative = -1e30


def attend_block(query_rows, query_pos, block_kv, key_pos, scale):
    scores = (
        lax.dot_general(
            query_rows, block_kv[0], (((1,), (1,)), ((), ())), preferred_element_type=jnp.float32
        )
        * scale
    )
    visible = key_pos[None, :] <= query_pos[:, None]
    return (jnp.where(visible, scores, big_negative), visible)


def sweep(step_fn, states, key_piece, offset, positions):
    span_size = key_piece.shape[1]
    block_size = math.gcd(span_size, 1024)

    def step(step_index, inner):
        block_kv = lax.dynamic_slice_in_dim(key_piece, step_index * block_size, block_size, 1)
        key_pos = lax.dynamic_slice_in_dim(
            positions, offset + step_index * block_size, block_size, 0
        )
        return step_fn(inner, block_kv, key_pos)

    return lax.fori_loop(0, span_size // block_size, step, states)


def wide_body(queries, keys_values, out_weight, out_grad, positions):
    token_count = queries.shape[0]
    head_count = queries.shape[1] // HD
    scale = HD ** (-0.5)
    seq_index = lax.axis_index("seq")
    head_index = lax.axis_index("head")
    kv_group = head_index * head_count // GROUP
    own_kv = lax.dynamic_slice_in_dim(keys_values, kv_group * HD, HD, 2)
    own_pos = lax.dynamic_slice_in_dim(positions, seq_index * token_count, token_count, 0)
    query_pos = jnp.repeat(own_pos, head_count)
    query_rows = queries.reshape(token_count * head_count, HD)
    d_attn = jnp.einsum(
        "td,dhc->thc",
        out_grad,
        lax.all_to_all(out_weight, "head", split_axis=1, concat_axis=0, tiled=True),
        preferred_element_type=jnp.float32,
    )
    d_attn = d_attn.astype(jnp.bfloat16).reshape(token_count * head_count, HD)
    row_total = token_count * head_count
    zeros_col = jnp.zeros((row_total, 1), jnp.float32)
    zeros_rows = jnp.zeros((row_total, HD), jnp.float32)
    lowest_col = jnp.full((row_total, 1), big_negative, jnp.float32)
    all_kv = lax.all_gather(own_kv, "seq", axis=1, tiled=True)

    def run_sweep(step_fn, init):
        return sweep(step_fn, init, all_kv, 0, positions)

    def stats_step(states, block_kv, key_pos):
        top, norm = states
        scores, visible = attend_block(query_rows, query_pos, block_kv, key_pos, scale)
        new_top = jnp.maximum(top, jnp.max(scores, axis=1, keepdims=True))
        weights = jnp.where(visible, jnp.exp(scores - new_top), 0.0)
        norm = jnp.exp(top - new_top) * norm + jnp.sum(weights, axis=1, keepdims=True)
        return (new_top, norm)

    top, norm = run_sweep(stats_step, (lowest_col, zeros_col))

    def block_probs(block_kv, key_pos):
        scores, visible = attend_block(query_rows, query_pos, block_kv, key_pos, scale)
        return jnp.where(visible, jnp.exp(scores - top), 0.0) / norm

    def out_step(acc_out, block_kv, key_pos):
        probs = block_probs(block_kv, key_pos)
        return acc_out + jnp.dot(
            probs.astype(jnp.bfloat16), block_kv[1], preferred_element_type=jnp.float32
        )

    attn_full = run_sweep(out_step, zeros_rows)
    delta = jnp.sum(d_attn.astype(jnp.float32) * attn_full, axis=1, keepdims=True)

    def grad_step(acc_grad, block_kv, key_pos):
        probs = block_probs(block_kv, key_pos)
        dprob = lax.dot_general(
            d_attn, block_kv[1], (((1,), (1,)), ((), ())), preferred_element_type=jnp.float32
        )
        dscore = (probs * (dprob - delta)).astype(jnp.bfloat16)
        return acc_grad + jnp.dot(dscore, block_kv[0], preferred_element_type=jnp.float32)

    d_rows = run_sweep(grad_step, zeros_rows) * scale
    attn = attn_full.astype(jnp.bfloat16).reshape(token_count, head_count, HD)
    d_query = d_rows.astype(jnp.bfloat16).reshape(token_count, head_count * HD)
    d_out_weight = lax.psum_scatter(
        jnp.einsum("td,thc->dhc", out_grad, attn, preferred_element_type=jnp.float32),
        "seq",
        scatter_dimension=0,
        tiled=True,
    )
    return (d_query, d_out_weight)


bf16, f32 = jnp.bfloat16, jnp.float32
ROWS = (((1,), (1,)), ((), ()))
COLS = (((0,), (0,)), ((), ()))


def dot(left, right, dims=(((1,), (0,)), ((), ()))):
    return lax.dot_general(left, right, dims, preferred_element_type=f32)


def xor_pairs(size, mask):
    return [(index, index ^ mask) for index in range(size)]


def vmem_call(kernel, outs, flops, limit, *args, scratch=()):
    return pl.pallas_call(
        kernel,
        out_shape=[pltpu.VMEM(shape, dtype) for shape, dtype in outs],
        in_specs=[pl.BlockSpec(memory_space=pltpu.VMEM)] * len(args),
        out_specs=[pl.BlockSpec(memory_space=pltpu.VMEM)] * len(outs),
        scratch_shapes=[pltpu.VMEM(shape, dtype) for shape, dtype in scratch],
        cost_estimate=pl.CostEstimate(flops=flops, bytes_accessed=1 << 16, transcendentals=0),
        compiler_params=pltpu.CompilerParams(vmem_limit_bytes=limit << 20),
    )(*args)


def pack_kernel(kv_ref, query_ref, out_ref, sems):
    copies = [
        pltpu.make_async_copy(source, out_ref.at[:, cols], sems.at[index])
        for index, (source, cols) in enumerate(
            (
                (kv_ref.at[0], slice(0, HD)),
                (kv_ref.at[1], slice(HD, 2 * HD)),
                (query_ref, slice(2 * HD, out_ref.shape[1])),
            )
        )
    ]
    for copy in copies:
        copy.start()
    for copy in copies:
        copy.wait()


def slice_kernel(grad_ref, *out_refs):
    pair = lax.axis_index("seq") // 2
    span = out_refs[0].shape[1]
    for mask, out_ref in enumerate(out_refs):
        start = pl.multiple_of((pair ^ mask) * span, 128)
        out_ref[...] = grad_ref[:, pl.ds(start, span)]


def split_masks(masks, bit):
    kept = [mask for mask in masks if not mask & bit]
    return kept, [mask | bit for mask in kept]


def parts_kernel(grad_ref, weight_ref, kept_ref, sent_ref, flat):
    rows, heads, _ = weight_ref.shape
    head = lax.axis_index("head")
    flat[...] = weight_ref[...].reshape(rows * heads, HD).astype(f32)
    cols = grad_ref[:, pl.ds(pl.multiple_of(head * rows, 128), rows)]
    size = lax.axis_size("head")
    per = heads // size
    for out_ref, masks in zip((kept_ref, sent_ref), split_masks(range(size), 1)):
        for place, mask in enumerate(masks):
            for h in range(per):
                weight = flat[pl.ds((head ^ mask) * per + h, rows, stride=heads), :].astype(bf16)
                start = (place * per + h) * HD
                out_ref[:, start : start + HD] = dot(cols, weight).astype(out_ref.dtype)


def blend_kernel(width, bit, kept_ref, got_ref, next_ref, sent_ref):
    masks = [mask for mask in range(lax.axis_size("head")) if not mask & (bit - 1)]
    for out_ref, chosen in zip((next_ref, sent_ref), split_masks(masks, bit)):
        for place, mask in enumerate(chosen):
            cols = slice(masks.index(mask) * width, (masks.index(mask) + 1) * width)
            total = kept_ref[:, cols] + got_ref[:, cols].astype(f32)
            out_ref[:, place * width : (place + 1) * width] = total.astype(out_ref.dtype)


def join_kernel(*refs):
    token_refs, out_ref = refs[:-1], refs[-1]
    rows = token_refs[0].shape[0]
    for block, ref in enumerate(token_refs):
        out_ref[block * rows : (block + 1) * rows, :] = ref[:, : 2 * HD]


def attention_kernel(pos_ref, near_ref, far_ref, *refs):
    token_refs, (attn_ref, full_ref, prob_ref, score_ref, weight_ref) = refs[:-5], refs[-5:]
    rows = token_refs[0].shape[0]
    blocks = len(token_refs)
    half = blocks * rows
    seq = lax.axis_index("seq")
    pair, low = seq // 2, seq % 2
    places = [
        pos_ref[pl.ds(2 * (pair ^ mask) + side, 1), :]
        for side in (low, 1 - low)
        for mask in range(blocks)
    ]
    key_pos = jnp.concatenate(places, axis=1)
    row_id = lax.broadcasted_iota(jnp.int32, (rows, rows), 0)
    col_id = lax.broadcasted_iota(jnp.int32, (rows, rows), 1)
    heads = range(score_ref.shape[0])
    for h in heads:
        query = jnp.concatenate([ref[:, (2 + h) * HD : (3 + h) * HD] for ref in token_refs], axis=0)
        score_ref[h, :, :half] = dot(query, near_ref[:, :HD], ROWS)
        score_ref[h, :, half:] = dot(query, far_ref[:, :HD], ROWS)
    for h in heads:
        cols = slice(h * HD, (h + 1) * HD)
        shares = []
        for block in range(blocks):
            span = slice(block * rows, (block + 1) * rows)
            query_pos = jnp.sum(
                jnp.where(row_id == col_id, places[block], 0), axis=1, keepdims=True
            )
            scores = jnp.where(key_pos <= query_pos, score_ref[h, span, :], big_negative)
            top = jnp.max(scores, axis=1, keepdims=True)
            weights = jnp.exp2((scores - top) * (HD ** (-0.5) * math.log2(math.e)))
            shares.append(1.0 / jnp.sum(weights, axis=1, keepdims=True))
            weight_ref[h, span, :] = weights.astype(bf16)
            if block == 0:
                prob_ref[h] = weights * shares[0]
        full = dot(weight_ref[h, :, :half], near_ref[:, HD:])
        full = full + dot(weight_ref[h, :, half:], far_ref[:, HD:])
        full = full * jnp.concatenate(shares, axis=0)
        attn_ref[:, cols] = full.astype(bf16)
        full_ref[:, cols] = full[:rows]


def query_kernel(near_ref, far_ref, full_ref, prob_ref, kept_ref, got_ref, out_ref):
    d_attn = (kept_ref[...] + got_ref[...].astype(f32)).astype(bf16)
    half = near_ref.shape[0]
    for h in range(prob_ref.shape[0]):
        cols = slice(h * HD, (h + 1) * HD)
        grad = d_attn[:, cols]
        delta = jnp.sum(grad.astype(f32) * full_ref[:, cols], axis=1, keepdims=True)
        acc = 0.0
        for side, ref in enumerate((near_ref, far_ref)):
            dprob = dot(grad, ref[:, HD:], ROWS)
            prob = prob_ref[h, :, side * half : (side + 1) * half]
            acc = acc + dot((prob * (dprob - delta)).astype(bf16), ref[:, :HD])
        out_ref[:, cols] = (acc * HD ** (-0.5)).astype(bf16)


def sums_kernel(attn_ref, *refs):
    grad_refs, (mine_ref, theirs_ref) = refs[:-2], refs[-2:]
    low = lax.axis_index("seq") % 2
    grads = jnp.concatenate([ref[...] for ref in grad_refs], axis=0)
    sums = dot(grads, attn_ref[...], COLS)
    half = sums.shape[0] // 2
    mine_ref[...] = jnp.where(low == 0, sums[:half], sums[half:])
    theirs = jnp.where(low == 0, sums[half:], sums[:half])
    theirs_ref[...] = theirs.astype(theirs_ref.dtype)


def add_kernel(mine_ref, theirs_ref, out_ref):
    for h in range(out_ref.shape[1]):
        cols = slice(h * HD, (h + 1) * HD)
        out_ref[:, h, :] = mine_ref[:, cols] + theirs_ref[:, cols].astype(f32)


def narrow_body(queries, keys_values, out_weight, out_grad, positions, seq_size, head_size):
    token_count = queries.shape[0]
    head_count = queries.shape[1] // HD
    width = head_count * HD
    head_index = lax.axis_index("head")
    pair_count = seq_size // 2
    span = out_grad.shape[1] // pair_count
    rows_in = out_weight.shape[0]
    tokens_near = pair_count * token_count
    if keys_values.shape[2] == HD:
        own_kv = keys_values
    else:
        own_kv = lax.dynamic_slice_in_dim(keys_values, head_index * head_count // GROUP * HD, HD, 2)

    def move(array, axis, size, mask):
        return lax.ppermute(array, axis, xor_pairs(size, mask))

    masks = range(1, pair_count)
    own_tokens = pl.pallas_call(
        pack_kernel,
        out_shape=pltpu.VMEM((token_count, 2 * HD + width), bf16),
        in_specs=[pl.BlockSpec(memory_space=pltpu.HBM)] * 2,
        out_specs=pl.BlockSpec(memory_space=pltpu.VMEM),
        scratch_shapes=[pltpu.SemaphoreType.DMA((3,))],
        cost_estimate=pl.CostEstimate(flops=1 << 32, bytes_accessed=1 << 18, transcendentals=0),
        compiler_params=pltpu.CompilerParams(vmem_limit_bytes=2 << 20),
    )(
        pltpu.with_memory_space_constraint(own_kv, pltpu.HBM),
        pltpu.with_memory_space_constraint(queries, pltpu.HBM),
    )
    tokens = [own_tokens] + [move(own_tokens, "seq", seq_size, 2 * m) for m in masks]
    grads = vmem_call(
        slice_kernel, [((token_count, span), bf16)] * pair_count, 1 << 32, 4, out_grad
    )
    grads = [grads[0]] + [move(grads[m], "seq", seq_size, 2 * m) for m in masks]

    half = (token_count, head_size // 2 * width)
    kept, sent = vmem_call(
        parts_kernel,
        [(half, f32), (half, bf16)],
        1 << 28,
        16,
        out_grad,
        out_weight,
        scratch=[((rows_in * out_weight.shape[1], HD), f32)],
    )
    got = move(sent, "head", head_size, 1)
    bit = 2
    while bit < head_size:
        half = (token_count, kept.shape[1] // 2)
        kept, sent = vmem_call(
            functools.partial(blend_kernel, width, bit),
            [(half, f32), (half, bf16)],
            1 << 20,
            2,
            kept,
            got,
        )
        got = move(sent, "head", head_size, bit)
        bit *= 2

    (near,) = vmem_call(join_kernel, [((tokens_near, 2 * HD), bf16)], 1 << 20, 2, *tokens)
    far = move(near, "seq", seq_size, 1)
    attn, full, prob = vmem_call(
        attention_kernel,
        [
            ((tokens_near, width), bf16),
            ((token_count, width), f32),
            ((head_count, token_count, 2 * tokens_near), f32),
        ],
        1 << 29,
        24,
        positions.reshape(seq_size, token_count),
        near,
        far,
        *tokens,
        scratch=[
            ((head_count, tokens_near, 2 * tokens_near), kind) for kind in (f32, bf16)
        ],
    )
    mine, theirs = vmem_call(
        sums_kernel,
        [((span // 2, width), kind) for kind in (f32, bf16)],
        1 << 28,
        12,
        attn,
        *grads,
    )
    theirs = move(theirs, "seq", seq_size, 1)
    (d_query,) = vmem_call(
        query_kernel,
        [((token_count, width), bf16)],
        1 << 28,
        8,
        near,
        far,
        full,
        prob,
        kept,
        got,
    )
    d_out_weight = pl.pallas_call(
        add_kernel,
        out_shape=jax.ShapeDtypeStruct((span // 2, head_count, HD), f32),
        cost_estimate=pl.CostEstimate(flops=1 << 20, bytes_accessed=1 << 20, transcendentals=0),
        compiler_params=pltpu.CompilerParams(vmem_limit_bytes=4 << 20),
    )(mine, theirs)
    return (d_query, d_out_weight)


def solution(mesh):
    seq_size, head_size = mesh.shape["seq"], mesh.shape["head"]
    narrow = seq_size == 8 and head_size in (2, 4, 8)

    def body(*arrays):
        if not narrow:
            return wide_body(*arrays)
        return narrow_body(*arrays, seq_size, head_size)

    return jax.shard_map(
        body,
        mesh=mesh,
        in_specs=(
            P("seq", "head"),
            P(None, "seq", None),
            P("head", None, None),
            P("seq", None),
            P(),
        ),
        out_specs=(P("seq", "head"), P("seq", "head", None)),
        check_vma=False,
    )
```

```python
import functools
import math

import jax
import jax.numpy as jnp
from jax import lax
from jax.experimental import pallas as pl
from jax.experimental.pallas import tpu as pltpu
from jax.sharding import PartitionSpec as P


HD = 128
GROUP = 8


big_negative = -1e30


def attend_block(query_rows, query_pos, block_kv, key_pos, scale):
    scores = (
        lax.dot_general(
            query_rows, block_kv[0], (((1,), (1,)), ((), ())), preferred_element_type=jnp.float32
        )
        * scale
    )
    visible = key_pos[None, :] <= query_pos[:, None]
    return (jnp.where(visible, scores, big_negative), visible)


def sweep(step_fn, states, key_piece, offset, positions):
    span_size = key_piece.shape[1]
    block_size = math.gcd(span_size, 1024)

    def step(step_index, inner):
        block_kv = lax.dynamic_slice_in_dim(key_piece, step_index * block_size, block_size, 1)
        key_pos = lax.dynamic_slice_in_dim(
            positions, offset + step_index * block_size, block_size, 0
        )
        return step_fn(inner, block_kv, key_pos)

    return lax.fori_loop(0, span_size // block_size, step, states)


def wide_body(queries, keys_values, out_weight, out_grad, positions):
    token_count = queries.shape[0]
    head_count = queries.shape[1] // HD
    scale = HD ** (-0.5)
    seq_index = lax.axis_index("seq")
    head_index = lax.axis_index("head")
    kv_group = head_index * head_count // GROUP
    own_kv = lax.dynamic_slice_in_dim(keys_values, kv_group * HD, HD, 2)
    own_pos = lax.dynamic_slice_in_dim(positions, seq_index * token_count, token_count, 0)
    query_pos = jnp.repeat(own_pos, head_count)
    query_rows = queries.reshape(token_count * head_count, HD)
    d_attn = jnp.einsum(
        "td,dhc->thc",
        out_grad,
        lax.all_to_all(out_weight, "head", split_axis=1, concat_axis=0, tiled=True),
        preferred_element_type=jnp.float32,
    )
    d_attn = d_attn.astype(jnp.bfloat16).reshape(token_count * head_count, HD)
    row_total = token_count * head_count
    zeros_col = jnp.zeros((row_total, 1), jnp.float32)
    zeros_rows = jnp.zeros((row_total, HD), jnp.float32)
    lowest_col = jnp.full((row_total, 1), big_negative, jnp.float32)
    all_kv = lax.all_gather(own_kv, "seq", axis=1, tiled=True)

    def run_sweep(step_fn, init):
        return sweep(step_fn, init, all_kv, 0, positions)

    def stats_step(states, block_kv, key_pos):
        top, norm = states
        scores, visible = attend_block(query_rows, query_pos, block_kv, key_pos, scale)
        new_top = jnp.maximum(top, jnp.max(scores, axis=1, keepdims=True))
        weights = jnp.where(visible, jnp.exp(scores - new_top), 0.0)
        norm = jnp.exp(top - new_top) * norm + jnp.sum(weights, axis=1, keepdims=True)
        return (new_top, norm)

    top, norm = run_sweep(stats_step, (lowest_col, zeros_col))

    def block_probs(block_kv, key_pos):
        scores, visible = attend_block(query_rows, query_pos, block_kv, key_pos, scale)
        return jnp.where(visible, jnp.exp(scores - top), 0.0) / norm

    def out_step(acc_out, block_kv, key_pos):
        probs = block_probs(block_kv, key_pos)
        return acc_out + jnp.dot(
            probs.astype(jnp.bfloat16), block_kv[1], preferred_element_type=jnp.float32
        )

    attn_full = run_sweep(out_step, zeros_rows)
    delta = jnp.sum(d_attn.astype(jnp.float32) * attn_full, axis=1, keepdims=True)

    def grad_step(acc_grad, block_kv, key_pos):
        probs = block_probs(block_kv, key_pos)
        dprob = lax.dot_general(
            d_attn, block_kv[1], (((1,), (1,)), ((), ())), preferred_element_type=jnp.float32
        )
        dscore = (probs * (dprob - delta)).astype(jnp.bfloat16)
        return acc_grad + jnp.dot(dscore, block_kv[0], preferred_element_type=jnp.float32)

    d_rows = run_sweep(grad_step, zeros_rows) * scale
    attn = attn_full.astype(jnp.bfloat16).reshape(token_count, head_count, HD)
    d_query = d_rows.astype(jnp.bfloat16).reshape(token_count, head_count * HD)
    d_out_weight = lax.psum_scatter(
        jnp.einsum("td,thc->dhc", out_grad, attn, preferred_element_type=jnp.float32),
        "seq",
        scatter_dimension=0,
        tiled=True,
    )
    return (d_query, d_out_weight)


bf16, f32 = jnp.bfloat16, jnp.float32
ROWS = (((1,), (1,)), ((), ()))
COLS = (((0,), (0,)), ((), ()))


def dot(left, right, dims=(((1,), (0,)), ((), ()))):
    return lax.dot_general(left, right, dims, preferred_element_type=f32)


def xor_pairs(size, mask):
    return [(index, index ^ mask) for index in range(size)]


def vmem_call(kernel, outs, flops, limit, *args, scratch=()):
    return pl.pallas_call(
        kernel,
        out_shape=[pltpu.VMEM(shape, dtype) for shape, dtype in outs],
        in_specs=[pl.BlockSpec(memory_space=pltpu.VMEM)] * len(args),
        out_specs=[pl.BlockSpec(memory_space=pltpu.VMEM)] * len(outs),
        scratch_shapes=[pltpu.VMEM(shape, dtype) for shape, dtype in scratch],
        cost_estimate=pl.CostEstimate(flops=flops, bytes_accessed=1 << 16, transcendentals=0),
        compiler_params=pltpu.CompilerParams(vmem_limit_bytes=limit << 20),
    )(*args)


def pack_kernel(kv_ref, query_ref, out_ref, sems):
    copies = [
        pltpu.make_async_copy(source, out_ref.at[:, cols], sems.at[index])
        for index, (source, cols) in enumerate(
            (
                (kv_ref.at[0], slice(0, HD)),
                (kv_ref.at[1], slice(HD, 2 * HD)),
                (query_ref, slice(2 * HD, out_ref.shape[1])),
            )
        )
    ]
    for copy in copies:
        copy.start()
    for copy in copies:
        copy.wait()


def slice_kernel(grad_ref, *out_refs):
    pair = lax.axis_index("seq") // 2
    span = out_refs[0].shape[1]
    for mask, out_ref in enumerate(out_refs):
        start = pl.multiple_of((pair ^ mask) * span, 128)
        out_ref[...] = grad_ref[:, pl.ds(start, span)]


def split_masks(masks, bit):
    kept = [mask for mask in masks if not mask & bit]
    return kept, [mask | bit for mask in kept]


def parts_kernel(grad_ref, weight_ref, kept_ref, sent_ref, flat):
    rows, heads, _ = weight_ref.shape
    head = lax.axis_index("head")
    flat[...] = weight_ref[...].reshape(rows * heads, HD).astype(f32)
    cols = grad_ref[:, pl.ds(pl.multiple_of(head * rows, 128), rows)]
    size = lax.axis_size("head")
    per = heads // size
    for out_ref, masks in zip((kept_ref, sent_ref), split_masks(range(size), 1)):
        for place, mask in enumerate(masks):
            for h in range(per):
                weight = flat[pl.ds((head ^ mask) * per + h, rows, stride=heads), :].astype(bf16)
                start = (place * per + h) * HD
                out_ref[:, start : start + HD] = dot(cols, weight).astype(out_ref.dtype)


def blend_kernel(width, bit, kept_ref, got_ref, next_ref, sent_ref):
    masks = [mask for mask in range(lax.axis_size("head")) if not mask & (bit - 1)]
    for out_ref, chosen in zip((next_ref, sent_ref), split_masks(masks, bit)):
        for place, mask in enumerate(chosen):
            cols = slice(masks.index(mask) * width, (masks.index(mask) + 1) * width)
            total = kept_ref[:, cols] + got_ref[:, cols].astype(f32)
            out_ref[:, place * width : (place + 1) * width] = total.astype(out_ref.dtype)


def join_kernel(*refs):
    token_refs, out_ref = refs[:-1], refs[-1]
    rows = token_refs[0].shape[0]
    for block, ref in enumerate(token_refs):
        out_ref[block * rows : (block + 1) * rows, :] = ref[:, : 2 * HD]


def attention_kernel(pos_ref, near_ref, far_ref, *refs):
    token_refs, (attn_ref, full_ref, prob_ref, score_ref, weight_ref) = refs[:-5], refs[-5:]
    rows = token_refs[0].shape[0]
    blocks = len(token_refs)
    half = blocks * rows
    seq = lax.axis_index("seq")
    pair, low = seq // 2, seq % 2
    places = [
        pos_ref[pl.ds(2 * (pair ^ mask) + side, 1), :]
        for side in (low, 1 - low)
        for mask in range(blocks)
    ]
    key_pos = jnp.concatenate(places, axis=1)
    row_id = lax.broadcasted_iota(jnp.int32, (rows, rows), 0)
    col_id = lax.broadcasted_iota(jnp.int32, (rows, rows), 1)
    heads = range(score_ref.shape[0])
    for h in heads:
        query = jnp.concatenate([ref[:, (2 + h) * HD : (3 + h) * HD] for ref in token_refs], axis=0)
        score_ref[h, :, :half] = dot(query, near_ref[:, :HD], ROWS)
        score_ref[h, :, half:] = dot(query, far_ref[:, :HD], ROWS)
    for h in heads:
        cols = slice(h * HD, (h + 1) * HD)
        shares = []
        for block in range(blocks):
            span = slice(block * rows, (block + 1) * rows)
            query_pos = jnp.sum(
                jnp.where(row_id == col_id, places[block], 0), axis=1, keepdims=True
            )
            scores = jnp.where(key_pos <= query_pos, score_ref[h, span, :], big_negative)
            top = jnp.max(scores, axis=1, keepdims=True)
            weights = jnp.exp2((scores - top) * (HD ** (-0.5) * math.log2(math.e)))
            shares.append(1.0 / jnp.sum(weights, axis=1, keepdims=True))
            weight_ref[h, span, :] = weights.astype(bf16)
            if block == 0:
                prob_ref[h] = weights * shares[0]
        full = dot(weight_ref[h, :, :half], near_ref[:, HD:])
        full = full + dot(weight_ref[h, :, half:], far_ref[:, HD:])
        full = full * jnp.concatenate(shares, axis=0)
        attn_ref[:, cols] = full.astype(bf16)
        full_ref[:, cols] = full[:rows]


def query_kernel(near_ref, far_ref, full_ref, prob_ref, kept_ref, got_ref, out_ref):
    d_attn = (kept_ref[...] + got_ref[...].astype(f32)).astype(bf16)
    half = near_ref.shape[0]
    for h in range(prob_ref.shape[0]):
        cols = slice(h * HD, (h + 1) * HD)
        grad = d_attn[:, cols]
        delta = jnp.sum(grad.astype(f32) * full_ref[:, cols], axis=1, keepdims=True)
        acc = 0.0
        for side, ref in enumerate((near_ref, far_ref)):
            dprob = dot(grad, ref[:, HD:], ROWS)
            prob = prob_ref[h, :, side * half : (side + 1) * half]
            acc = acc + dot((prob * (dprob - delta)).astype(bf16), ref[:, :HD])
        out_ref[:, cols] = (acc * HD ** (-0.5)).astype(bf16)


def early_kernel(attn_ref, first_ref, last_ref, acc_ref):
    rows = first_ref.shape[0]
    grads = jnp.concatenate([first_ref[...], last_ref[...]], axis=0)
    attn = jnp.concatenate([attn_ref[:rows, :], attn_ref[-rows:, :]], axis=0)
    acc_ref[...] = dot(grads, attn, COLS)


def late_kernel(own, acc_ref, attn_ref, *refs):
    grad_refs, (out_ref, sum_ref) = refs[:-2], refs[-2:]
    rows, half = grad_refs[0].shape[0], out_ref.shape[0]
    low = lax.axis_index("seq") % 2
    side = low if own else 1 - low
    base = half // 128 * 128
    size = 2 * half - base
    cols = pl.ds(pl.multiple_of(side * base, 128), size)
    grads = jnp.concatenate([ref[:, cols] for ref in grad_refs], axis=0)
    sum_ref[...] = dot(grads, attn_ref[rows : rows + grads.shape[0], :], COLS)
    late = sum_ref[pl.ds(pl.multiple_of(side * (half - base), 8), half), :]
    early = acc_ref[pl.ds(pl.multiple_of(side * half, 8), half), :]
    out_ref[...] = (early + late).astype(out_ref.dtype)


def add_kernel(mine_ref, theirs_ref, query_ref, query_out, out_ref, sum_ref, sems):
    pieces = sems.shape[0] - 1
    rows = mine_ref.shape[0] // pieces
    copies = [pltpu.make_async_copy(query_ref, query_out, sems.at[pieces])]
    copies[0].start()
    for piece in range(pieces):
        span = slice(piece * rows, (piece + 1) * rows)
        for h in range(sum_ref.shape[1]):
            cols = slice(h * HD, (h + 1) * HD)
            sum_ref[span, h, :] = mine_ref[span, cols] + theirs_ref[span, cols].astype(f32)
        copies.append(pltpu.make_async_copy(sum_ref.at[span], out_ref.at[span], sems.at[piece]))
        if piece:
            copies[piece].start()
    copies[pieces].start()
    for copy in copies:
        copy.wait()


def narrow_body(queries, keys_values, out_weight, out_grad, positions, seq_size, head_size):
    token_count = queries.shape[0]
    head_count = queries.shape[1] // HD
    width = head_count * HD
    head_index = lax.axis_index("head")
    pair_count = seq_size // 2
    span = out_grad.shape[1] // pair_count
    rows_in = out_weight.shape[0]
    tokens_near = pair_count * token_count
    if keys_values.shape[2] == HD:
        own_kv = keys_values
    else:
        own_kv = lax.dynamic_slice_in_dim(keys_values, head_index * head_count // GROUP * HD, HD, 2)

    def move(array, axis, size, mask):
        return lax.ppermute(array, axis, xor_pairs(size, mask))

    masks = range(1, pair_count)
    own_tokens = pl.pallas_call(
        pack_kernel,
        out_shape=pltpu.VMEM((token_count, 2 * HD + width), bf16),
        in_specs=[pl.BlockSpec(memory_space=pltpu.HBM)] * 2,
        out_specs=pl.BlockSpec(memory_space=pltpu.VMEM),
        scratch_shapes=[pltpu.SemaphoreType.DMA((3,))],
        cost_estimate=pl.CostEstimate(flops=1 << 32, bytes_accessed=1 << 18, transcendentals=0),
        compiler_params=pltpu.CompilerParams(vmem_limit_bytes=2 << 20),
    )(
        pltpu.with_memory_space_constraint(own_kv, pltpu.HBM),
        pltpu.with_memory_space_constraint(queries, pltpu.HBM),
    )
    tokens = [own_tokens] + [move(own_tokens, "seq", seq_size, 2 * m) for m in masks]
    grads = vmem_call(
        slice_kernel, [((token_count, span), bf16)] * pair_count, 1 << 32, 4, out_grad
    )
    grads = [grads[0]] + [move(grads[m], "seq", seq_size, 2 * m) for m in masks]

    half = (token_count, head_size // 2 * width)
    kept, sent = vmem_call(
        parts_kernel,
        [(half, f32), (half, bf16)],
        1 << 28,
        16,
        out_grad,
        out_weight,
        scratch=[((rows_in * out_weight.shape[1], HD), f32)],
    )
    got = move(sent, "head", head_size, 1)
    bit = 2
    while bit < head_size:
        half = (token_count, kept.shape[1] // 2)
        kept, sent = vmem_call(
            functools.partial(blend_kernel, width, bit),
            [(half, f32), (half, bf16)],
            1 << 20,
            2,
            kept,
            got,
        )
        got = move(sent, "head", head_size, bit)
        bit *= 2

    (near,) = vmem_call(join_kernel, [((tokens_near, 2 * HD), bf16)], 1 << 20, 2, *tokens)
    far = move(near, "seq", seq_size, 1)
    attn, full, prob = vmem_call(
        attention_kernel,
        [
            ((tokens_near, width), bf16),
            ((token_count, width), f32),
            ((head_count, token_count, 2 * tokens_near), f32),
        ],
        1 << 29,
        24,
        positions.reshape(seq_size, token_count),
        near,
        far,
        *tokens,
        scratch=[
            ((head_count, tokens_near, 2 * tokens_near), kind) for kind in (f32, bf16)
        ],
    )
    (acc,) = vmem_call(early_kernel, [((span, width), f32)], 1 << 27, 6, attn, grads[0], grads[-1])
    half = span // 2
    scratch = [((span - half // 128 * 128, width), f32)]

    def late(own, kind):
        return vmem_call(
            functools.partial(late_kernel, own),
            [((half, width), kind)],
            1 << 27,
            6,
            acc,
            attn,
            *grads[1:-1],
            scratch=scratch,
        )

    (theirs,) = late(False, bf16)
    theirs = move(theirs, "seq", seq_size, 1)
    (mine,) = late(True, f32)
    (d_query,) = vmem_call(
        query_kernel,
        [((token_count, width), bf16)],
        1 << 28,
        8,
        near,
        far,
        full,
        prob,
        kept,
        got,
    )
    shape = (span // 2, head_count, HD)
    d_query, d_out_weight = pl.pallas_call(
        add_kernel,
        out_shape=[pltpu.HBM((token_count, width), bf16), pltpu.HBM(shape, f32)],
        in_specs=[pl.BlockSpec(memory_space=pltpu.VMEM)] * 3,
        out_specs=[pl.BlockSpec(memory_space=pltpu.HBM)] * 2,
        scratch_shapes=[pltpu.VMEM(shape, f32), pltpu.SemaphoreType.DMA((5,))],
        cost_estimate=pl.CostEstimate(flops=1 << 20, bytes_accessed=1 << 20, transcendentals=0),
        compiler_params=pltpu.CompilerParams(vmem_limit_bytes=4 << 20),
    )(mine, theirs, d_query)
    return (d_query, d_out_weight)


def solution(mesh):
    seq_size, head_size = mesh.shape["seq"], mesh.shape["head"]
    narrow = seq_size == 8 and head_size in (2, 4, 8)

    def body(*arrays):
        if not narrow:
            return wide_body(*arrays)
        return narrow_body(*arrays, seq_size, head_size)

    return jax.shard_map(
        body,
        mesh=mesh,
        in_specs=(
            P("seq", "head"),
            P(None, "seq", None),
            P("head", None, None),
            P("seq", None),
            P(),
        ),
        out_specs=(P("seq", "head"), P("seq", "head", None)),
        check_vma=False,
    )
```

```python
import functools
import math

import jax
import jax.numpy as jnp
from jax import lax
from jax.experimental import pallas as pl
from jax.experimental.pallas import tpu as pltpu
from jax.sharding import PartitionSpec as P


HD = 128
GROUP = 8


big_negative = -1e30


def attend_block(query_rows, query_pos, block_kv, key_pos, scale):
    scores = (
        lax.dot_general(
            query_rows, block_kv[0], (((1,), (1,)), ((), ())), preferred_element_type=jnp.float32
        )
        * scale
    )
    visible = key_pos[None, :] <= query_pos[:, None]
    return (jnp.where(visible, scores, big_negative), visible)


def sweep(step_fn, states, key_piece, offset, positions):
    span_size = key_piece.shape[1]
    block_size = math.gcd(span_size, 1024)

    def step(step_index, inner):
        block_kv = lax.dynamic_slice_in_dim(key_piece, step_index * block_size, block_size, 1)
        key_pos = lax.dynamic_slice_in_dim(
            positions, offset + step_index * block_size, block_size, 0
        )
        return step_fn(inner, block_kv, key_pos)

    return lax.fori_loop(0, span_size // block_size, step, states)


def wide_body(queries, keys_values, out_weight, out_grad, positions):
    token_count = queries.shape[0]
    head_count = queries.shape[1] // HD
    scale = HD ** (-0.5)
    seq_index = lax.axis_index("seq")
    head_index = lax.axis_index("head")
    kv_group = head_index * head_count // GROUP
    own_kv = lax.dynamic_slice_in_dim(keys_values, kv_group * HD, HD, 2)
    own_pos = lax.dynamic_slice_in_dim(positions, seq_index * token_count, token_count, 0)
    query_pos = jnp.repeat(own_pos, head_count)
    query_rows = queries.reshape(token_count * head_count, HD)
    d_attn = jnp.einsum(
        "td,dhc->thc",
        out_grad,
        lax.all_to_all(out_weight, "head", split_axis=1, concat_axis=0, tiled=True),
        preferred_element_type=jnp.float32,
    )
    d_attn = d_attn.astype(jnp.bfloat16).reshape(token_count * head_count, HD)
    row_total = token_count * head_count
    zeros_col = jnp.zeros((row_total, 1), jnp.float32)
    zeros_rows = jnp.zeros((row_total, HD), jnp.float32)
    lowest_col = jnp.full((row_total, 1), big_negative, jnp.float32)
    all_kv = lax.all_gather(own_kv, "seq", axis=1, tiled=True)

    def run_sweep(step_fn, init):
        return sweep(step_fn, init, all_kv, 0, positions)

    def stats_step(states, block_kv, key_pos):
        top, norm = states
        scores, visible = attend_block(query_rows, query_pos, block_kv, key_pos, scale)
        new_top = jnp.maximum(top, jnp.max(scores, axis=1, keepdims=True))
        weights = jnp.where(visible, jnp.exp(scores - new_top), 0.0)
        norm = jnp.exp(top - new_top) * norm + jnp.sum(weights, axis=1, keepdims=True)
        return (new_top, norm)

    top, norm = run_sweep(stats_step, (lowest_col, zeros_col))

    def block_probs(block_kv, key_pos):
        scores, visible = attend_block(query_rows, query_pos, block_kv, key_pos, scale)
        return jnp.where(visible, jnp.exp(scores - top), 0.0) / norm

    def out_step(acc_out, block_kv, key_pos):
        probs = block_probs(block_kv, key_pos)
        return acc_out + jnp.dot(
            probs.astype(jnp.bfloat16), block_kv[1], preferred_element_type=jnp.float32
        )

    attn_full = run_sweep(out_step, zeros_rows)
    delta = jnp.sum(d_attn.astype(jnp.float32) * attn_full, axis=1, keepdims=True)

    def grad_step(acc_grad, block_kv, key_pos):
        probs = block_probs(block_kv, key_pos)
        dprob = lax.dot_general(
            d_attn, block_kv[1], (((1,), (1,)), ((), ())), preferred_element_type=jnp.float32
        )
        dscore = (probs * (dprob - delta)).astype(jnp.bfloat16)
        return acc_grad + jnp.dot(dscore, block_kv[0], preferred_element_type=jnp.float32)

    d_rows = run_sweep(grad_step, zeros_rows) * scale
    attn = attn_full.astype(jnp.bfloat16).reshape(token_count, head_count, HD)
    d_query = d_rows.astype(jnp.bfloat16).reshape(token_count, head_count * HD)
    d_out_weight = lax.psum_scatter(
        jnp.einsum("td,thc->dhc", out_grad, attn, preferred_element_type=jnp.float32),
        "seq",
        scatter_dimension=0,
        tiled=True,
    )
    return (d_query, d_out_weight)


bf16, f32 = jnp.bfloat16, jnp.float32
ROWS = (((1,), (1,)), ((), ()))
COLS = (((0,), (0,)), ((), ()))


def dot(left, right, dims=(((1,), (0,)), ((), ()))):
    return lax.dot_general(left, right, dims, preferred_element_type=f32)


def xor_pairs(size, mask):
    return [(index, index ^ mask) for index in range(size)]


def vmem_call(kernel, outs, flops, limit, *args, scratch=()):
    return pl.pallas_call(
        kernel,
        out_shape=[pltpu.VMEM(shape, dtype) for shape, dtype in outs],
        in_specs=[pl.BlockSpec(memory_space=pltpu.VMEM)] * len(args),
        out_specs=[pl.BlockSpec(memory_space=pltpu.VMEM)] * len(outs),
        scratch_shapes=[pltpu.VMEM(shape, dtype) for shape, dtype in scratch],
        cost_estimate=pl.CostEstimate(flops=flops, bytes_accessed=1 << 16, transcendentals=0),
        compiler_params=pltpu.CompilerParams(vmem_limit_bytes=limit << 20),
    )(*args)


def pack_kernel(kv_ref, query_ref, out_ref, sems):
    copies = [
        pltpu.make_async_copy(source, out_ref.at[:, cols], sems.at[index])
        for index, (source, cols) in enumerate(
            (
                (kv_ref.at[0], slice(0, HD)),
                (kv_ref.at[1], slice(HD, 2 * HD)),
                (query_ref, slice(2 * HD, out_ref.shape[1])),
            )
        )
    ]
    for copy in copies:
        copy.start()
    for copy in copies:
        copy.wait()


def slice_kernel(grad_ref, *out_refs):
    pair = lax.axis_index("seq") // 2
    span = out_refs[0].shape[1]
    for mask, out_ref in enumerate(out_refs):
        start = pl.multiple_of((pair ^ mask) * span, 128)
        out_ref[...] = grad_ref[:, pl.ds(start, span)]


def split_masks(masks, bit):
    kept = [mask for mask in masks if not mask & bit]
    return kept, [mask | bit for mask in kept]


def parts_kernel(grad_ref, weight_ref, kept_ref, sent_ref, flat):
    rows, heads, _ = weight_ref.shape
    head = lax.axis_index("head")
    flat[...] = weight_ref[...].reshape(rows * heads, HD).astype(f32)
    cols = grad_ref[:, pl.ds(pl.multiple_of(head * rows, 128), rows)]
    size = lax.axis_size("head")
    per = heads // size
    for out_ref, masks in zip((kept_ref, sent_ref), split_masks(range(size), 1)):
        for place, mask in enumerate(masks):
            weights = [
                flat[pl.ds((head ^ mask) * per + h, rows, stride=heads), :].astype(bf16)
                for h in range(per)
            ]
            span = slice(place * per * HD, (place + 1) * per * HD)
            product = dot(cols, jnp.concatenate(weights, axis=1))
            out_ref[:, span] = product.astype(out_ref.dtype)


def blend_kernel(width, bit, kept_ref, got_ref, next_ref, sent_ref):
    masks = [mask for mask in range(lax.axis_size("head")) if not mask & (bit - 1)]
    for out_ref, chosen in zip((next_ref, sent_ref), split_masks(masks, bit)):
        for place, mask in enumerate(chosen):
            cols = slice(masks.index(mask) * width, (masks.index(mask) + 1) * width)
            total = kept_ref[:, cols] + got_ref[:, cols].astype(f32)
            out_ref[:, place * width : (place + 1) * width] = total.astype(out_ref.dtype)


def join_kernel(*refs):
    token_refs, out_ref = refs[:-1], refs[-1]
    rows = token_refs[0].shape[0]
    for block, ref in enumerate(token_refs):
        out_ref[block * rows : (block + 1) * rows, :] = ref[:, : 2 * HD]


def attention_kernel(pos_ref, near_ref, far_ref, *refs):
    token_refs, (attn_ref, full_ref, prob_ref, score_ref, weight_ref) = refs[:-5], refs[-5:]
    rows = token_refs[0].shape[0]
    blocks = len(token_refs)
    half = blocks * rows
    seq = lax.axis_index("seq")
    pair, low = seq // 2, seq % 2
    places = [
        pos_ref[pl.ds(2 * (pair ^ mask) + side, 1), :]
        for side in (low, 1 - low)
        for mask in range(blocks)
    ]
    key_pos = jnp.concatenate(places, axis=1)
    row_id = lax.broadcasted_iota(jnp.int32, (rows, rows), 0)
    col_id = lax.broadcasted_iota(jnp.int32, (rows, rows), 1)
    heads = range(score_ref.shape[0])
    for h in heads:
        query = jnp.concatenate([ref[:, (2 + h) * HD : (3 + h) * HD] for ref in token_refs], axis=0)
        score_ref[h, :, :half] = dot(query, near_ref[:, :HD], ROWS)
        score_ref[h, :, half:] = dot(query, far_ref[:, :HD], ROWS)
    for h in heads:
        cols = slice(h * HD, (h + 1) * HD)
        shares = []
        for block in range(blocks):
            span = slice(block * rows, (block + 1) * rows)
            query_pos = jnp.sum(
                jnp.where(row_id == col_id, places[block], 0), axis=1, keepdims=True
            )
            scores = jnp.where(key_pos <= query_pos, score_ref[h, span, :], big_negative)
            top = jnp.max(scores, axis=1, keepdims=True)
            weights = jnp.exp2((scores - top) * (HD ** (-0.5) * math.log2(math.e)))
            shares.append(1.0 / jnp.sum(weights, axis=1, keepdims=True))
            weight_ref[h, span, :] = weights.astype(bf16)
            if block == 0:
                prob_ref[h] = weights * shares[0]
        full = dot(weight_ref[h, :, :half], near_ref[:, HD:])
        full = full + dot(weight_ref[h, :, half:], far_ref[:, HD:])
        full = full * jnp.concatenate(shares, axis=0)
        attn_ref[:, cols] = full.astype(bf16)
        full_ref[:, cols] = full[:rows]


def query_kernel(near_ref, far_ref, full_ref, prob_ref, kept_ref, got_ref, out_ref):
    d_attn = (kept_ref[...] + got_ref[...].astype(f32)).astype(bf16)
    half = near_ref.shape[0]
    for h in range(prob_ref.shape[0]):
        cols = slice(h * HD, (h + 1) * HD)
        grad = d_attn[:, cols]
        delta = jnp.sum(grad.astype(f32) * full_ref[:, cols], axis=1, keepdims=True)
        acc = 0.0
        for side, ref in enumerate((near_ref, far_ref)):
            dprob = dot(grad, ref[:, HD:], ROWS)
            prob = prob_ref[h, :, side * half : (side + 1) * half]
            acc = acc + dot((prob * (dprob - delta)).astype(bf16), ref[:, :HD])
        out_ref[:, cols] = (acc * HD ** (-0.5)).astype(bf16)


def early_kernel(attn_ref, first_ref, last_ref, acc_ref):
    rows = first_ref.shape[0]
    grads = jnp.concatenate([first_ref[...], last_ref[...]], axis=0)
    attn = jnp.concatenate([attn_ref[:rows, :], attn_ref[-rows:, :]], axis=0)
    acc_ref[...] = dot(grads, attn, COLS)


def late_kernel(own, acc_ref, attn_ref, *refs):
    grad_refs, (out_ref, sum_ref) = refs[:-2], refs[-2:]
    rows, half = grad_refs[0].shape[0], out_ref.shape[0]
    low = lax.axis_index("seq") % 2
    side = low if own else 1 - low
    base = half // 128 * 128
    size = 2 * half - base
    cols = pl.ds(pl.multiple_of(side * base, 128), size)
    grads = jnp.concatenate([ref[:, cols] for ref in grad_refs], axis=0)
    sum_ref[...] = dot(grads, attn_ref[rows : rows + grads.shape[0], :], COLS)
    late = sum_ref[pl.ds(pl.multiple_of(side * (half - base), 8), half), :]
    early = acc_ref[pl.ds(pl.multiple_of(side * half, 8), half), :]
    out_ref[...] = (early + late).astype(out_ref.dtype)


def add_kernel(mine_ref, theirs_ref, query_ref, query_out, out_ref, sum_ref, sems):
    pieces = sems.shape[0] - 1
    rows = mine_ref.shape[0] // pieces
    copies = [pltpu.make_async_copy(query_ref, query_out, sems.at[pieces])]
    copies[0].start()
    for piece in range(pieces):
        span = slice(piece * rows, (piece + 1) * rows)
        for h in range(sum_ref.shape[1]):
            cols = slice(h * HD, (h + 1) * HD)
            sum_ref[span, h, :] = mine_ref[span, cols] + theirs_ref[span, cols].astype(f32)
        copies.append(pltpu.make_async_copy(sum_ref.at[span], out_ref.at[span], sems.at[piece]))
        if piece:
            copies[piece].start()
    copies[pieces].start()
    for copy in copies:
        copy.wait()


def narrow_body(queries, keys_values, out_weight, out_grad, positions, seq_size, head_size):
    token_count = queries.shape[0]
    head_count = queries.shape[1] // HD
    width = head_count * HD
    head_index = lax.axis_index("head")
    pair_count = seq_size // 2
    span = out_grad.shape[1] // pair_count
    rows_in = out_weight.shape[0]
    tokens_near = pair_count * token_count
    if keys_values.shape[2] == HD:
        own_kv = keys_values
    else:
        own_kv = lax.dynamic_slice_in_dim(keys_values, head_index * head_count // GROUP * HD, HD, 2)

    def move(array, axis, size, mask):
        return lax.ppermute(array, axis, xor_pairs(size, mask))

    masks = range(1, pair_count)
    own_tokens = pl.pallas_call(
        pack_kernel,
        out_shape=pltpu.VMEM((token_count, 2 * HD + width), bf16),
        in_specs=[pl.BlockSpec(memory_space=pltpu.HBM)] * 2,
        out_specs=pl.BlockSpec(memory_space=pltpu.VMEM),
        scratch_shapes=[pltpu.SemaphoreType.DMA((3,))],
        cost_estimate=pl.CostEstimate(flops=1 << 32, bytes_accessed=1 << 18, transcendentals=0),
        compiler_params=pltpu.CompilerParams(vmem_limit_bytes=2 << 20),
    )(
        pltpu.with_memory_space_constraint(own_kv, pltpu.HBM),
        pltpu.with_memory_space_constraint(queries, pltpu.HBM),
    )
    tokens = [own_tokens] + [move(own_tokens, "seq", seq_size, 2 * m) for m in masks]
    grads = vmem_call(
        slice_kernel, [((token_count, span), bf16)] * pair_count, 1 << 32, 4, out_grad
    )
    grads = [grads[0]] + [move(grads[m], "seq", seq_size, 2 * m) for m in masks]

    half = (token_count, head_size // 2 * width)
    kept, sent = vmem_call(
        parts_kernel,
        [(half, f32), (half, bf16)],
        1 << 28,
        16,
        out_grad,
        out_weight,
        scratch=[((rows_in * out_weight.shape[1], HD), f32)],
    )
    got = move(sent, "head", head_size, 1)
    bit = 2
    while bit < head_size:
        half = (token_count, kept.shape[1] // 2)
        kept, sent = vmem_call(
            functools.partial(blend_kernel, width, bit),
            [(half, f32), (half, bf16)],
            1 << 20,
            2,
            kept,
            got,
        )
        got = move(sent, "head", head_size, bit)
        bit *= 2

    (near,) = vmem_call(join_kernel, [((tokens_near, 2 * HD), bf16)], 1 << 20, 2, *tokens)
    far = move(near, "seq", seq_size, 1)
    attn, full, prob = vmem_call(
        attention_kernel,
        [
            ((tokens_near, width), bf16),
            ((token_count, width), f32),
            ((head_count, token_count, 2 * tokens_near), f32),
        ],
        1 << 29,
        24,
        positions.reshape(seq_size, token_count),
        near,
        far,
        *tokens,
        scratch=[
            ((head_count, tokens_near, 2 * tokens_near), kind) for kind in (f32, bf16)
        ],
    )
    (acc,) = vmem_call(early_kernel, [((span, width), f32)], 1 << 27, 6, attn, grads[0], grads[-1])
    half = span // 2
    scratch = [((span - half // 128 * 128, width), f32)]

    def late(own, kind):
        return vmem_call(
            functools.partial(late_kernel, own),
            [((half, width), kind)],
            1 << 27,
            6,
            acc,
            attn,
            *grads[1:-1],
            scratch=scratch,
        )

    (theirs,) = late(False, bf16)
    theirs = move(theirs, "seq", seq_size, 1)
    (mine,) = late(True, f32)
    (d_query,) = vmem_call(
        query_kernel,
        [((token_count, width), bf16)],
        1 << 28,
        8,
        near,
        far,
        full,
        prob,
        kept,
        got,
    )
    shape = (span // 2, head_count, HD)
    d_query, d_out_weight = pl.pallas_call(
        add_kernel,
        out_shape=[pltpu.HBM((token_count, width), bf16), pltpu.HBM(shape, f32)],
        in_specs=[pl.BlockSpec(memory_space=pltpu.VMEM)] * 3,
        out_specs=[pl.BlockSpec(memory_space=pltpu.HBM)] * 2,
        scratch_shapes=[pltpu.VMEM(shape, f32), pltpu.SemaphoreType.DMA((5,))],
        cost_estimate=pl.CostEstimate(flops=1 << 20, bytes_accessed=1 << 20, transcendentals=0),
        compiler_params=pltpu.CompilerParams(vmem_limit_bytes=4 << 20),
    )(mine, theirs, d_query)
    return (d_query, d_out_weight)


def solution(mesh):
    seq_size, head_size = mesh.shape["seq"], mesh.shape["head"]
    narrow = seq_size == 8 and head_size in (2, 4, 8)

    def body(*arrays):
        if not narrow:
            return wide_body(*arrays)
        return narrow_body(*arrays, seq_size, head_size)

    return jax.shard_map(
        body,
        mesh=mesh,
        in_specs=(
            P("seq", "head"),
            P(None, "seq", None),
            P("head", None, None),
            P("seq", None),
            P(),
        ),
        out_specs=(P("seq", "head"), P("seq", "head", None)),
        check_vma=False,
    )
```

```python
import functools
import math

import jax
import jax.numpy as jnp
from jax import lax
from jax.experimental import pallas as pl
from jax.experimental.pallas import tpu as pltpu
from jax.sharding import PartitionSpec as P


HD = 128
GROUP = 8


big_negative = -1e30


def attend_block(query_rows, query_pos, block_kv, key_pos, scale):
    scores = (
        lax.dot_general(
            query_rows, block_kv[0], (((1,), (1,)), ((), ())), preferred_element_type=jnp.float32
        )
        * scale
    )
    visible = key_pos[None, :] <= query_pos[:, None]
    return (jnp.where(visible, scores, big_negative), visible)


def sweep(step_fn, states, key_piece, offset, positions):
    span_size = key_piece.shape[1]
    block_size = math.gcd(span_size, 1024)

    def step(step_index, inner):
        block_kv = lax.dynamic_slice_in_dim(key_piece, step_index * block_size, block_size, 1)
        key_pos = lax.dynamic_slice_in_dim(
            positions, offset + step_index * block_size, block_size, 0
        )
        return step_fn(inner, block_kv, key_pos)

    return lax.fori_loop(0, span_size // block_size, step, states)


def wide_body(queries, keys_values, out_weight, out_grad, positions):
    token_count = queries.shape[0]
    head_count = queries.shape[1] // HD
    scale = HD ** (-0.5)
    seq_index = lax.axis_index("seq")
    head_index = lax.axis_index("head")
    kv_group = head_index * head_count // GROUP
    own_kv = lax.dynamic_slice_in_dim(keys_values, kv_group * HD, HD, 2)
    own_pos = lax.dynamic_slice_in_dim(positions, seq_index * token_count, token_count, 0)
    query_pos = jnp.repeat(own_pos, head_count)
    query_rows = queries.reshape(token_count * head_count, HD)
    d_attn = jnp.einsum(
        "td,dhc->thc",
        out_grad,
        lax.all_to_all(out_weight, "head", split_axis=1, concat_axis=0, tiled=True),
        preferred_element_type=jnp.float32,
    )
    d_attn = d_attn.astype(jnp.bfloat16).reshape(token_count * head_count, HD)
    row_total = token_count * head_count
    zeros_col = jnp.zeros((row_total, 1), jnp.float32)
    zeros_rows = jnp.zeros((row_total, HD), jnp.float32)
    lowest_col = jnp.full((row_total, 1), big_negative, jnp.float32)
    all_kv = lax.all_gather(own_kv, "seq", axis=1, tiled=True)

    def run_sweep(step_fn, init):
        return sweep(step_fn, init, all_kv, 0, positions)

    def stats_step(states, block_kv, key_pos):
        top, norm = states
        scores, visible = attend_block(query_rows, query_pos, block_kv, key_pos, scale)
        new_top = jnp.maximum(top, jnp.max(scores, axis=1, keepdims=True))
        weights = jnp.where(visible, jnp.exp(scores - new_top), 0.0)
        norm = jnp.exp(top - new_top) * norm + jnp.sum(weights, axis=1, keepdims=True)
        return (new_top, norm)

    top, norm = run_sweep(stats_step, (lowest_col, zeros_col))

    def block_probs(block_kv, key_pos):
        scores, visible = attend_block(query_rows, query_pos, block_kv, key_pos, scale)
        return jnp.where(visible, jnp.exp(scores - top), 0.0) / norm

    def out_step(acc_out, block_kv, key_pos):
        probs = block_probs(block_kv, key_pos)
        return acc_out + jnp.dot(
            probs.astype(jnp.bfloat16), block_kv[1], preferred_element_type=jnp.float32
        )

    attn_full = run_sweep(out_step, zeros_rows)
    delta = jnp.sum(d_attn.astype(jnp.float32) * attn_full, axis=1, keepdims=True)

    def grad_step(acc_grad, block_kv, key_pos):
        probs = block_probs(block_kv, key_pos)
        dprob = lax.dot_general(
            d_attn, block_kv[1], (((1,), (1,)), ((), ())), preferred_element_type=jnp.float32
        )
        dscore = (probs * (dprob - delta)).astype(jnp.bfloat16)
        return acc_grad + jnp.dot(dscore, block_kv[0], preferred_element_type=jnp.float32)

    d_rows = run_sweep(grad_step, zeros_rows) * scale
    attn = attn_full.astype(jnp.bfloat16).reshape(token_count, head_count, HD)
    d_query = d_rows.astype(jnp.bfloat16).reshape(token_count, head_count * HD)
    d_out_weight = lax.psum_scatter(
        jnp.einsum("td,thc->dhc", out_grad, attn, preferred_element_type=jnp.float32),
        "seq",
        scatter_dimension=0,
        tiled=True,
    )
    return (d_query, d_out_weight)


bf16, f32 = jnp.bfloat16, jnp.float32
ROWS = (((1,), (1,)), ((), ()))
COLS = (((0,), (0,)), ((), ()))


def dot(left, right, dims=(((1,), (0,)), ((), ()))):
    return lax.dot_general(left, right, dims, preferred_element_type=f32)


def xor_pairs(size, mask):
    return [(index, index ^ mask) for index in range(size)]


def vmem_call(kernel, outs, flops, limit, *args, scratch=()):
    return pl.pallas_call(
        kernel,
        out_shape=[pltpu.VMEM(shape, dtype) for shape, dtype in outs],
        in_specs=[pl.BlockSpec(memory_space=pltpu.VMEM)] * len(args),
        out_specs=[pl.BlockSpec(memory_space=pltpu.VMEM)] * len(outs),
        scratch_shapes=[pltpu.VMEM(shape, dtype) for shape, dtype in scratch],
        cost_estimate=pl.CostEstimate(flops=flops, bytes_accessed=1 << 16, transcendentals=0),
        compiler_params=pltpu.CompilerParams(vmem_limit_bytes=limit << 20),
    )(*args)


def pack_kernel(kv_ref, query_ref, out_ref, sems):
    pieces = sems.shape[1]
    rows = out_ref.shape[0] // pieces
    copies = []
    for piece in range(pieces):
        span = slice(piece * rows, (piece + 1) * rows)
        for index, (source, cols) in enumerate(
            (
                (kv_ref.at[0, span], slice(0, HD)),
                (kv_ref.at[1, span], slice(HD, 2 * HD)),
                (query_ref.at[span], slice(2 * HD, out_ref.shape[1])),
            )
        ):
            copies.append(
                pltpu.make_async_copy(source, out_ref.at[span, cols], sems.at[index, piece])
            )
    for copy in copies:
        copy.start()
    for copy in copies:
        copy.wait()


def slice_kernel(grad_ref, *out_refs):
    pair = lax.axis_index("seq") // 2
    span = out_refs[0].shape[1]
    for mask, out_ref in enumerate(out_refs):
        start = pl.multiple_of((pair ^ mask) * span, 128)
        out_ref[...] = grad_ref[:, pl.ds(start, span)]


def split_masks(masks, bit):
    kept = [mask for mask in masks if not mask & bit]
    return kept, [mask | bit for mask in kept]


def parts_kernel(grad_ref, weight_ref, kept_ref, sent_ref, flat):
    rows, heads, _ = weight_ref.shape
    head = lax.axis_index("head")
    flat[...] = weight_ref[...].reshape(rows * heads, HD).astype(f32)
    cols = grad_ref[:, pl.ds(pl.multiple_of(head * rows, 128), rows)]
    size = lax.axis_size("head")
    per = heads // size
    for out_ref, masks in zip((kept_ref, sent_ref), split_masks(range(size), 1)):
        for place, mask in enumerate(masks):
            weights = [
                flat[pl.ds((head ^ mask) * per + h, rows, stride=heads), :].astype(bf16)
                for h in range(per)
            ]
            span = slice(place * per * HD, (place + 1) * per * HD)
            product = dot(cols, jnp.concatenate(weights, axis=1))
            out_ref[:, span] = product.astype(out_ref.dtype)


def blend_kernel(width, bit, kept_ref, got_ref, next_ref, sent_ref):
    masks = [mask for mask in range(lax.axis_size("head")) if not mask & (bit - 1)]
    for out_ref, chosen in zip((next_ref, sent_ref), split_masks(masks, bit)):
        for place, mask in enumerate(chosen):
            cols = slice(masks.index(mask) * width, (masks.index(mask) + 1) * width)
            total = kept_ref[:, cols] + got_ref[:, cols].astype(f32)
            out_ref[:, place * width : (place + 1) * width] = total.astype(out_ref.dtype)


def join_kernel(*refs):
    token_refs, out_ref = refs[:-1], refs[-1]
    rows = token_refs[0].shape[0]
    for block, ref in enumerate(token_refs):
        out_ref[block * rows : (block + 1) * rows, :] = ref[:, : 2 * HD]


def attention_kernel(pos_ref, near_ref, far_ref, *refs):
    token_refs, (attn_ref, full_ref, prob_ref, score_ref, weight_ref) = refs[:-5], refs[-5:]
    rows = token_refs[0].shape[0]
    blocks = len(token_refs)
    half = blocks * rows
    seq = lax.axis_index("seq")
    pair, low = seq // 2, seq % 2
    places = [
        pos_ref[pl.ds(2 * (pair ^ mask) + side, 1), :]
        for side in (low, 1 - low)
        for mask in range(blocks)
    ]
    key_pos = jnp.concatenate(places, axis=1)
    row_id = lax.broadcasted_iota(jnp.int32, (rows, rows), 0)
    col_id = lax.broadcasted_iota(jnp.int32, (rows, rows), 1)
    heads = range(score_ref.shape[0])
    for h in heads:
        query = jnp.concatenate([ref[:, (2 + h) * HD : (3 + h) * HD] for ref in token_refs], axis=0)
        score_ref[h, :, :half] = dot(query, near_ref[:, :HD], ROWS)
        score_ref[h, :, half:] = dot(query, far_ref[:, :HD], ROWS)
    for h in heads:
        cols = slice(h * HD, (h + 1) * HD)
        shares = []
        for block in range(blocks):
            span = slice(block * rows, (block + 1) * rows)
            query_pos = jnp.sum(
                jnp.where(row_id == col_id, places[block], 0), axis=1, keepdims=True
            )
            scores = jnp.where(key_pos <= query_pos, score_ref[h, span, :], big_negative)
            top = jnp.max(scores, axis=1, keepdims=True)
            weights = jnp.exp2((scores - top) * (HD ** (-0.5) * math.log2(math.e)))
            shares.append(1.0 / jnp.sum(weights, axis=1, keepdims=True))
            weight_ref[h, span, :] = weights.astype(bf16)
            if block == 0:
                prob_ref[h] = weights * shares[0]
        full = dot(weight_ref[h, :, :half], near_ref[:, HD:])
        full = full + dot(weight_ref[h, :, half:], far_ref[:, HD:])
        full = full * jnp.concatenate(shares, axis=0)
        attn_ref[:, cols] = full.astype(bf16)
        full_ref[:, cols] = full[:rows]


def query_kernel(near_ref, far_ref, full_ref, prob_ref, kept_ref, got_ref, out_ref):
    d_attn = (kept_ref[...] + got_ref[...].astype(f32)).astype(bf16)
    half = near_ref.shape[0]
    for h in range(prob_ref.shape[0]):
        cols = slice(h * HD, (h + 1) * HD)
        grad = d_attn[:, cols]
        delta = jnp.sum(grad.astype(f32) * full_ref[:, cols], axis=1, keepdims=True)
        acc = 0.0
        for side, ref in enumerate((near_ref, far_ref)):
            dprob = dot(grad, ref[:, HD:], ROWS)
            prob = prob_ref[h, :, side * half : (side + 1) * half]
            acc = acc + dot((prob * (dprob - delta)).astype(bf16), ref[:, :HD])
        out_ref[:, cols] = (acc * HD ** (-0.5)).astype(bf16)


def early_kernel(attn_ref, first_ref, last_ref, acc_ref):
    rows = first_ref.shape[0]
    grads = jnp.concatenate([first_ref[...], last_ref[...]], axis=0)
    attn = jnp.concatenate([attn_ref[:rows, :], attn_ref[-rows:, :]], axis=0)
    acc_ref[...] = dot(grads, attn, COLS)


def late_kernel(own, acc_ref, attn_ref, *refs):
    grad_refs, (out_ref, sum_ref) = refs[:-2], refs[-2:]
    rows, half = grad_refs[0].shape[0], out_ref.shape[0]
    low = lax.axis_index("seq") % 2
    side = low if own else 1 - low
    base = half // 128 * 128
    size = 2 * half - base
    cols = pl.ds(pl.multiple_of(side * base, 128), size)
    grads = jnp.concatenate([ref[:, cols] for ref in grad_refs], axis=0)
    sum_ref[...] = dot(grads, attn_ref[rows : rows + grads.shape[0], :], COLS)
    late = sum_ref[pl.ds(pl.multiple_of(side * (half - base), 8), half), :]
    early = acc_ref[pl.ds(pl.multiple_of(side * half, 8), half), :]
    out_ref[...] = (early + late).astype(out_ref.dtype)


def add_kernel(mine_ref, theirs_ref, query_ref, query_out, out_ref, sum_ref, sems):
    pieces = sems.shape[0] - 1
    rows = mine_ref.shape[0] // pieces
    copies = [pltpu.make_async_copy(query_ref, query_out, sems.at[pieces])]
    copies[0].start()
    for piece in range(pieces):
        span = slice(piece * rows, (piece + 1) * rows)
        for h in range(sum_ref.shape[1]):
            cols = slice(h * HD, (h + 1) * HD)
            sum_ref[span, h, :] = mine_ref[span, cols] + theirs_ref[span, cols].astype(f32)
        copies.append(pltpu.make_async_copy(sum_ref.at[span], out_ref.at[span], sems.at[piece]))
        if piece:
            copies[piece].start()
    copies[pieces].start()
    for copy in copies:
        copy.wait()


def narrow_body(queries, keys_values, out_weight, out_grad, positions, seq_size, head_size):
    token_count = queries.shape[0]
    head_count = queries.shape[1] // HD
    width = head_count * HD
    head_index = lax.axis_index("head")
    pair_count = seq_size // 2
    span = out_grad.shape[1] // pair_count
    rows_in = out_weight.shape[0]
    tokens_near = pair_count * token_count
    if keys_values.shape[2] == HD:
        own_kv = keys_values
    else:
        own_kv = lax.dynamic_slice_in_dim(keys_values, head_index * head_count // GROUP * HD, HD, 2)

    def move(array, axis, size, mask):
        return lax.ppermute(array, axis, xor_pairs(size, mask))

    masks = range(1, pair_count)
    own_tokens = pl.pallas_call(
        pack_kernel,
        out_shape=pltpu.VMEM((token_count, 2 * HD + width), bf16),
        in_specs=[pl.BlockSpec(memory_space=pltpu.HBM)] * 2,
        out_specs=pl.BlockSpec(memory_space=pltpu.VMEM),
        scratch_shapes=[pltpu.SemaphoreType.DMA((3, 2))],
        cost_estimate=pl.CostEstimate(flops=1 << 32, bytes_accessed=1 << 18, transcendentals=0),
        compiler_params=pltpu.CompilerParams(vmem_limit_bytes=2 << 20),
    )(
        pltpu.with_memory_space_constraint(own_kv, pltpu.HBM),
        pltpu.with_memory_space_constraint(queries, pltpu.HBM),
    )
    tokens = [own_tokens] + [move(own_tokens, "seq", seq_size, 2 * m) for m in masks]
    grads = vmem_call(
        slice_kernel, [((token_count, span), bf16)] * pair_count, 1 << 32, 4, out_grad
    )
    grads = [grads[0]] + [move(grads[m], "seq", seq_size, 2 * m) for m in masks]

    half = (token_count, head_size // 2 * width)
    kept, sent = vmem_call(
        parts_kernel,
        [(half, f32), (half, bf16)],
        1 << 28,
        16,
        out_grad,
        out_weight,
        scratch=[((rows_in * out_weight.shape[1], HD), f32)],
    )
    got = move(sent, "head", head_size, 1)
    bit = 2
    while bit < head_size:
        half = (token_count, kept.shape[1] // 2)
        kept, sent = vmem_call(
            functools.partial(blend_kernel, width, bit),
            [(half, f32), (half, bf16)],
            1 << 20,
            2,
            kept,
            got,
        )
        got = move(sent, "head", head_size, bit)
        bit *= 2

    (near,) = vmem_call(join_kernel, [((tokens_near, 2 * HD), bf16)], 1 << 20, 2, *tokens)
    far = move(near, "seq", seq_size, 1)
    attn, full, prob = vmem_call(
        attention_kernel,
        [
            ((tokens_near, width), bf16),
            ((token_count, width), f32),
            ((head_count, token_count, 2 * tokens_near), f32),
        ],
        1 << 29,
        24,
        positions.reshape(seq_size, token_count),
        near,
        far,
        *tokens,
        scratch=[
            ((head_count, tokens_near, 2 * tokens_near), kind) for kind in (f32, bf16)
        ],
    )
    (acc,) = vmem_call(early_kernel, [((span, width), f32)], 1 << 27, 6, attn, grads[0], grads[-1])
    half = span // 2
    scratch = [((span - half // 128 * 128, width), f32)]

    def late(own, kind):
        return vmem_call(
            functools.partial(late_kernel, own),
            [((half, width), kind)],
            1 << 27,
            6,
            acc,
            attn,
            *grads[1:-1],
            scratch=scratch,
        )

    (theirs,) = late(False, bf16)
    theirs = move(theirs, "seq", seq_size, 1)
    (mine,) = late(True, f32)
    (d_query,) = vmem_call(
        query_kernel,
        [((token_count, width), bf16)],
        1 << 28,
        8,
        near,
        far,
        full,
        prob,
        kept,
        got,
    )
    shape = (span // 2, head_count, HD)
    d_query, d_out_weight = pl.pallas_call(
        add_kernel,
        out_shape=[pltpu.HBM((token_count, width), bf16), pltpu.HBM(shape, f32)],
        in_specs=[pl.BlockSpec(memory_space=pltpu.VMEM)] * 3,
        out_specs=[pl.BlockSpec(memory_space=pltpu.HBM)] * 2,
        scratch_shapes=[pltpu.VMEM(shape, f32), pltpu.SemaphoreType.DMA((5,))],
        cost_estimate=pl.CostEstimate(flops=1 << 20, bytes_accessed=1 << 20, transcendentals=0),
        compiler_params=pltpu.CompilerParams(vmem_limit_bytes=4 << 20),
    )(mine, theirs, d_query)
    return (d_query, d_out_weight)


def solution(mesh):
    seq_size, head_size = mesh.shape["seq"], mesh.shape["head"]
    narrow = seq_size == 8 and head_size in (2, 4, 8)

    def body(*arrays):
        if not narrow:
            return wide_body(*arrays)
        return narrow_body(*arrays, seq_size, head_size)

    return jax.shard_map(
        body,
        mesh=mesh,
        in_specs=(
            P("seq", "head"),
            P(None, "seq", None),
            P("head", None, None),
            P("seq", None),
            P(),
        ),
        out_specs=(P("seq", "head"), P("seq", "head", None)),
        check_vma=False,
    )
```
